512 devices in a mesh: dp: 64 (over z, x, core), tensor: 8 (over y).
Axes of the slice: x: 4, y: 8, z: 8, core: 2. Of those that a mesh axis runs over, the one named last changes fastest.
Arguments:
- residual: bfloat16 [16384, 4096], P('dp', 'tensor'), may hold values from -6 to 6
- fresh_qkv: bfloat16 [16384, 3, 2048], P('dp', None, 'tensor'), may hold values from -110 to 110
- active: int32 [16384], P('dp'), may hold values from 0 to 1
- home_slot: int32 [16384], P('dp'), may hold values from 0 to 16383, as said below
- kv_cache: bfloat16 [16384, 2, 16, 2048], P('dp', None, None, 'tensor'), may hold values from -6 to 6
- lengths: int32 [16384], P('dp'), may hold values from 2 to 16
- w_out: bfloat16 [2048, 4096], P('tensor'), may hold values from -0.125 to 0.125
Outputs:
- updated: bfloat16 [16384, 4096], P('dp', 'tensor')
The draws below stay inside these ranges and needn't reach their ends.
Inputs may be any that keep to these rules, and one draw needn't show every extreme that they name: Each dp group owns the slots 256 * g to 256 * g + 255; home_slot is a permutation. Among the streams of one dp group, at most 4 active streams have slots in the same owning group, and this is reached in every draw.
All inputs are finite; a program needn't handle non-finite values.
Results may differ from the reference program's by a relative error of at most 0.0062.
Values may be sent and summed in bfloat16 or wider, within the bound.
A program may use at most 64 MiB of HBM per device.

```python
import jax
import jax.numpy as jnp
from jax import lax

D = 4096
HEADS = 16
HD = 128
S_DEV = 256
L = 16
CAP = 4
STREAMS = 16384


def routing(key):
    base = jax.random.fold_in(key, 101)
    groups = STREAMS // S_DEV
    stream_index = jnp.arange(STREAMS, dtype=jnp.int32)
    source = stream_index // S_DEV
    within = stream_index % S_DEV
    shuffled = jax.random.permutation(jax.random.fold_in(base, 1), groups).astype(jnp.int32)
    inverse = jnp.argsort(shuffled).astype(jnp.int32)
    values = jnp.arange(groups, dtype=jnp.int32)
    priority = jnp.where(values == 1, 0, jnp.where(values == groups - 1, 1, jnp.where(values == groups // 2, 2, 3 + inverse)))
    offsets = jnp.argsort(priority).astype(jnp.int32)[:S_DEV // CAP]
    owner_group = (source + offsets[within // CAP]) % groups
    ranking = jax.random.randint(jax.random.fold_in(base, 2), (groups, S_DEV), 0, 1 << 20) * S_DEV + jnp.arange(S_DEV, dtype=jnp.int32)[None, :]
    slot_order = jnp.argsort(ranking, axis=1).astype(jnp.int32)
    home_slot = owner_group * S_DEV + slot_order[owner_group, within]
    active_level = jax.random.randint(jax.random.fold_in(base, 3), (groups,), 2, 9)
    dice_roll = jax.random.randint(jax.random.fold_in(base, 4), (STREAMS,), 0, 8)
    active = jnp.logical_or(dice_roll < active_level[owner_group], stream_index < CAP)
    return (home_slot.astype(jnp.int32), active.astype(jnp.int32))


def draw_home_slot(key, part):
    return routing(key)[0]


def draw_active(key, part):
    return routing(key)[1]


def draw_fresh_qkv(key, part):
    drawn = jnp.clip(jax.random.normal(jax.random.fold_in(key, 201), (STREAMS, 3, HEADS * HD), jnp.float32), -6.0, 6.0)
    return drawn.astype(jnp.bfloat16)


def draw_kv_cache(key, part):
    drawn = jnp.clip(jax.random.normal(jax.random.fold_in(key, 202), (STREAMS, 2, L, HEADS * HD), jnp.float32), -6.0, 6.0)
    return drawn.astype(jnp.bfloat16)


def place_ends(array, stream_key, least, top_value):
    longest = array.shape.index(max(array.shape))
    spots = []
    for shift in (0, 1):
        where = [jax.random.randint(jax.random.fold_in(stream_key, axis), (), 0, length) for axis, length in enumerate(array.shape)]
        where[longest] = (where[longest] + shift) % array.shape[longest]
        spots.append(tuple(where))
    return array.at[spots[0]].set(least).at[spots[1]].set(top_value)


def level_of(own_key, shape, shards, least, largest):
    factor_of = 1.0
    for position, shards_of in shards:
        draws = jax.random.uniform(jax.random.fold_in(jax.random.fold_in(own_key, 6), position), (shards_of,), jnp.float32, least / len(shards), largest / len(shards))
        factor_of = factor_of * jnp.repeat(jnp.exp(draws), shape[position] // shards_of).reshape((-1,) + (1,) * (len(shape) - 1 - position))
    return factor_of


def bell_draw(own_key, extent, width, most, split=(), held_as=jnp.bfloat16):
    result = jax.random.normal(own_key, extent, jnp.float32) * width
    if len(split) > 0:
        result = level_of(own_key, extent, split, -0.22, 0.18) * result
    return jnp.clip(result, min=-most, max=most).astype(held_as)


def setup_inputs(seed: int = 0) -> dict:
    keys = jax.random.split(jax.random.key(seed), 8)
    return {
        "residual": bell_draw(keys[0], (STREAMS, D), 1.0, 6.0, ((0, 64), (1, 8))),
        "fresh_qkv": draw_fresh_qkv(jax.random.fold_in(keys[7], 71), 0),
        "active": draw_active(jax.random.fold_in(keys[7], 71), 0),
        "home_slot": draw_home_slot(jax.random.fold_in(keys[7], 71), 0),
        "kv_cache": draw_kv_cache(jax.random.fold_in(keys[7], 71), 0),
        "lengths": place_ends(jax.random.randint(keys[5], (STREAMS,), 2, L + 1), jax.random.fold_in(keys[5], 1), 2, L).astype(jnp.int32),
        "w_out": bell_draw(keys[6], (HEADS * HD, D), (HEADS * HD) ** -0.5, 0.125, ((0, 8),)),
    }


def attend(query, key_rows, value_rows, key_new, value_new, length):
    score_scale = HD ** -0.5
    scores = jnp.einsum("bhd,blhd->bhl", query.astype(jnp.float32), key_rows.astype(jnp.float32)) * score_scale
    positions = jnp.arange(L, dtype=jnp.int32)
    in_cache = positions[None, None, :] < length[:, None, None]
    scores = jnp.where(in_cache, scores, jnp.float32(-1e30))
    own_score = jnp.sum(query.astype(jnp.float32) * key_new.astype(jnp.float32), axis=-1) * score_scale
    row_max = jnp.maximum(jnp.max(scores, axis=-1), own_score)
    weights_raw = jnp.exp(scores - row_max[..., None])
    own_raw = jnp.exp(own_score - row_max)
    denominator = jnp.sum(weights_raw, axis=-1) + own_raw
    weights = (weights_raw / denominator[..., None]).astype(jnp.bfloat16)
    own_weight = (own_raw / denominator).astype(jnp.bfloat16)
    mixed = jnp.einsum("bhl,blhd->bhd", weights.astype(jnp.float32), value_rows.astype(jnp.float32))
    mixed = mixed + own_weight.astype(jnp.float32)[..., None] * value_new.astype(jnp.float32)
    return mixed.astype(jnp.bfloat16).reshape(query.shape[0], -1)


def reference(residual, fresh_qkv, active, home_slot, kv_cache, lengths, w_out):
    groups = STREAMS // S_DEV

    def one_group(group):
        start = (group * S_DEV).astype(jnp.int32)
        streams = start + jnp.arange(S_DEV, dtype=jnp.int32)
        slots = home_slot[streams]
        fresh_rows = jnp.take(fresh_qkv, streams, axis=0).reshape(S_DEV, 3, HEADS, HD)
        cache_rows = jnp.take(kv_cache, slots, axis=0).reshape(S_DEV, 2, L, HEADS, HD)
        attended = attend(fresh_rows[:, 0], cache_rows[:, 0], cache_rows[:, 1], fresh_rows[:, 1], fresh_rows[:, 2], lengths[slots])
        projected = jnp.dot(attended, w_out, preferred_element_type=jnp.float32)
        rows = lax.dynamic_slice_in_dim(residual, start, S_DEV, 0).astype(jnp.float32)
        flags = active[streams].astype(jnp.float32)
        return (rows + flags[:, None] * projected).astype(jnp.bfloat16)

    updated = lax.map(one_group, jnp.arange(groups, dtype=jnp.int32))
    return updated.reshape(STREAMS, D)
```

```python
import functools

import jax
import jax.numpy as jnp
from jax import lax
from jax.experimental import pallas as pl
from jax.experimental.pallas import tpu as pltpu
from jax.sharding import PartitionSpec as P

MESH = pl.DeviceIdType.MESH
HD = 128
CAP = 4
F32, BF16, I32 = jnp.float32, jnp.bfloat16, jnp.int32


def dot(a, b, ca=1, cb=0):
    return lax.dot_general(a, b, (((ca,), (cb,)), ((), ())), preferred_element_type=F32)


def kernel(
    groups, ring,
    fresh_hbm, act_ref, home_ref, len_ref, kv_hbm, w_hbm, res_hbm,
    out_ref,
    fresh, kv, wcol, res, ids_s, ids_r, send, recv, rsend, rrecv, gath, place, match, owned, score, att, acc,
    lsem, ids_ss, ids_rs, dat_ss, dat_rs, ret_ss, ret_rs,
    wy_s, wy_r, wc_s, wc_r, wx_s, wx_r, wz_s, wz_r, agr_s, agr_r, agl_s, agl_r,
):
    n = act_ref.shape[1]
    length = kv.shape[2]
    cols = wcol.shape[2]
    depth = wcol.shape[1]
    me = lax.axis_index("dp")
    y = lax.axis_index("tensor")
    core = lax.rem(me, 2)
    xbit = lax.rem(me // 2, 2)
    partner = me + 1 - 2 * core
    across = me + 2 - 4 * xbit
    quarter = depth // 4

    def dp_peer(k):
        return lax.rem(me + k, groups)

    def y_peer(d):
        return lax.rem(y + d, ring)

    fresh_cp = pltpu.make_async_copy(fresh_hbm, fresh, lsem.at[0])
    fresh_cp.start()

    barrier = pltpu.get_barrier_semaphore()

    def greet(k, c):
        pl.semaphore_signal(barrier, inc=1, device_id={"dp": dp_peer(k)}, device_id_type=MESH)
        return c

    lax.fori_loop(1, groups, greet, 0)
    for d in range(1, ring):
        pl.semaphore_signal(barrier, inc=1, device_id={"tensor": y_peer(d)}, device_id_type=MESH)

    kv_cp = pltpu.make_async_copy(kv_hbm, kv, lsem.at[1])
    kv_cp.start()
    wown_cp = pltpu.make_async_copy(
        w_hbm.at[:, pl.ds(pl.multiple_of(y * cols, cols), cols)], wcol.at[y], lsem.at[2])
    wown_cp.start()
    res_cp = pltpu.make_async_copy(res_hbm, res, lsem.at[3])
    res_cp.start()

    home = home_ref[...]
    active = act_ref[...] > 0
    owner = home // n
    local_id = (home - owner * n + 1).astype(F32)
    of_group = (owner == lax.broadcasted_iota(I32, (groups, n), 0)) & active
    one_hot = jnp.where(of_group, 1.0, 0.0).astype(F32)
    before = jnp.where(
        lax.broadcasted_iota(I32, (n, n), 0) < lax.broadcasted_iota(I32, (n, n), 1), 1.0, 0.0
    ).astype(BF16)
    earlier = dot(one_hot.astype(BF16), before)
    rank = jnp.sum(one_hot * earlier, axis=0, keepdims=True)
    lane = lax.broadcasted_iota(I32, (groups, 128), 1)
    mine = (lane // 8) == lax.rem(me, 16)
    id_rows = jnp.zeros((groups, 128), F32)
    for r in range(CAP):
        value = jnp.sum(jnp.where(rank == r, one_hot * local_id, 0.0), axis=1, keepdims=True)
        id_rows = jnp.where(mine & (lane % 4 == r), value, id_rows)
    ids_s[...] = id_rows.reshape(groups, 1, 128)
    target = jnp.where(active, owner * 8 + rank.astype(I32), -64)
    spot = lax.broadcasted_iota(I32, (groups * 8, n), 0)
    for h in range(2):
        place[h] = jnp.where(spot == target + 4 * h, 1.0, 0.0).astype(BF16)
    fresh_cp.wait()
    for k in range(3):
        rows = dot(place[0], fresh[k, :, 0:HD]) + dot(place[1], fresh[k, :, HD:2 * HD])
        send[:, :, k * HD:(k + 1) * HD] = rows.astype(BF16).reshape(groups, 8, HD)

    pl.semaphore_wait(barrier, groups - 1 + ring - 1)

    def ids_copy(k):
        to = dp_peer(k)
        return pltpu.make_async_remote_copy(
            ids_s.at[to], ids_r.at[me], ids_ss, ids_rs, device_id={"dp": to}, device_id_type=MESH)

    def dat_copy(k):
        to = dp_peer(k)
        return pltpu.make_async_remote_copy(
            send.at[to], recv.at[me], dat_ss, dat_rs, device_id={"dp": to}, device_id_type=MESH)

    def ret_copy(k):
        to = dp_peer(k)
        return pltpu.make_async_remote_copy(
            rsend.at[to], rrecv.at[me], ret_ss, ret_rs, device_id={"dp": to}, device_id_type=MESH)

    def whole(src, dst, ss, rs):
        return pltpu.make_async_remote_copy(
            src.at[pl.ds(0, groups - 1)], dst.at[pl.ds(0, groups - 1)], ss, rs,
            device_id={"dp": partner}, device_id_type=MESH)

    def go(k, c):
        ids_copy(k).start()
        dat_copy(k).start()
        return c

    lax.fori_loop(1, groups, go, 0)
    own_ids = pltpu.make_async_copy(ids_s.at[me], ids_r.at[me], lsem.at[4])
    own_ids.start()
    own_dat = pltpu.make_async_copy(send.at[me], recv.at[me], lsem.at[5])
    own_dat.start()

    def part(cbit, xb):
        return pl.ds(pl.multiple_of((xb * 2 + cbit) * quarter, quarter), quarter)

    mypart = part(core, xbit)
    otherpart = part(core, 1 - xbit)
    order = [1, 7, 2, 6, 3, 5, 4]

    def wy_copy(d):
        to = y_peer(d)
        return pltpu.make_async_remote_copy(
            w_hbm.at[mypart, pl.ds(pl.multiple_of(to * cols, cols), cols)], wcol.at[y, mypart],
            wy_s.at[d], wy_r.at[d], device_id={"tensor": to}, device_id_type=MESH)

    def fwd_copy(d, rows, ss, rs, to):
        src = lax.rem(y + ring - d, ring)
        return pltpu.make_async_remote_copy(
            wcol.at[src, rows], wcol.at[src, rows], ss.at[d], rs.at[d],
            device_id={"dp": to}, device_id_type=MESH)

    def wc_copy(d):
        return fwd_copy(d, mypart, wc_s, wc_r, partner)

    def wx_copy(d):
        return fwd_copy(d, mypart, wx_s, wx_r, across)

    def wz_copy(d):
        return fwd_copy(d, otherpart, wz_s, wz_r, partner)

    for d in order:
        wy_copy(d).start()

    def pass_on(d):
        wy_copy(d).wait_recv()
        wx_copy(d).start()
        wc_copy(d).start()

    def pass_twice(d):
        wx_copy(d).wait_recv()
        wz_copy(d).start()

    for d in order[:4]:
        pass_on(d)

    own_ids.wait()
    own_dat.wait()
    whole(ids_s, ids_r, ids_ss, ids_rs).wait_recv()
    slot = lax.broadcasted_iota(I32, (n, 128), 0) + 1
    half = (lax.broadcasted_iota(I32, (n, 128), 1) % 8) // 4
    for b in range(groups // 16):
        ids = ids_r[16 * b]
        for i in range(1, 16):
            ids = ids + ids_r[16 * b + i]
        hit = ids.astype(I32) == slot
        for h in range(2):
            match[h, :, b * 128:(b + 1) * 128] = jnp.where(hit & (half == h), 1.0, 0.0).astype(BF16)
    len_row = len_ref[...]
    eye = lax.broadcasted_iota(I32, (n, n), 0) == lax.broadcasted_iota(I32, (n, n), 1)
    lengths = dot(jnp.where(eye, len_row, 0).astype(BF16), jnp.ones((n, 16 * length), BF16))
    whole(send, recv, dat_ss, dat_rs).wait_recv()
    for k in range(3):
        rows = recv[:, :, k * HD:(k + 1) * HD].reshape(groups * 8, HD)
        for h in range(2):
            owned[h, :, k * HD:(k + 1) * HD] = dot(match[h], rows).astype(BF16)

    kv_cp.wait()
    blocks = n // 16
    for h in range(2):
        cl = pl.ds(h * HD, HD)
        for i in range(blocks):
            keys = kv[16 * i:16 * i + 16, 0, :, cl].reshape(16 * length, HD)
            score[16 * i:16 * i + 16] = dot(owned[h, 16 * i:16 * i + 16, 0:HD], keys, 1, 1)
        scale = HD ** -0.5
        lane_i = lax.broadcasted_iota(I32, (n, 16 * length), 1)
        row_i = lax.broadcasted_iota(I32, (n, 16 * length), 0)
        valid = (lane_i // length == row_i % 16) & ((lane_i % length).astype(F32) < lengths)
        s = jnp.where(valid, score[...] * scale, -1e30)
        q = owned[h, :, 0:HD].astype(F32)
        own = jnp.sum(q * owned[h, :, HD:2 * HD].astype(F32), axis=1, keepdims=True) * scale
        top = jnp.maximum(jnp.max(s, axis=1, keepdims=True), own)
        e = jnp.where(valid, jnp.exp(s - top), 0.0)
        own_e = jnp.exp(own - top)
        z = jnp.sum(e, axis=1, keepdims=True) + own_e
        w = (e / z).astype(BF16)
        own_w = (own_e / z).astype(BF16).astype(F32)
        for i in range(blocks):
            values = kv[16 * i:16 * i + 16, 1, :, cl].reshape(16 * length, HD)
            mixed = dot(w[16 * i:16 * i + 16], values)
            fresh_v = owned[h, 16 * i:16 * i + 16, 2 * HD:3 * HD].astype(F32)
            mixed = mixed + own_w[16 * i:16 * i + 16] * fresh_v
            att[h, 16 * i:16 * i + 16] = mixed.astype(BF16)
    back = dot(match[0], att[0], 0, 0) + dot(match[1], att[1], 0, 0)
    rsend[...] = back.astype(BF16).reshape(groups, 8, HD)

    def go_back(k, c):
        ret_copy(k).start()
        return c

    lax.fori_loop(1, groups, go_back, 0)
    own_ret = pltpu.make_async_copy(rsend.at[me], rrecv.at[me], lsem.at[6])
    own_ret.start()

    for d in order[4:]:
        pass_on(d)
    for d in order:
        pass_twice(d)

    own_ret.wait()
    whole(rsend, rrecv, ret_ss, ret_rs).wait_recv()
    back_rows = rrecv[...].reshape(groups * 8, HD)
    for h in range(2):
        gath[y, :, h * HD:(h + 1) * HD] = dot(place[h], back_rows, 0, 0).astype(BF16)

    hr = n // 2

    def ring_copy(s, hf, way):
        src = lax.rem(y + (ring - s if way > 0 else s), ring)
        to = lax.rem(y + (1 if way > 0 else ring - 1), ring)
        ss, rs = (agr_s, agr_r) if way > 0 else (agl_s, agl_r)
        piece = gath.at[src, pl.ds(hf * hr, hr)]
        return pltpu.make_async_remote_copy(
            piece, piece, ss.at[2 * s + hf], rs.at[2 * s + hf],
            device_id={"tensor": to}, device_id_type=MESH)

    last = ring // 2 - 1
    moves = [(s, hf, way) for s in range(last + 1) for hf, way in ((0, 1), (1, -1), (1, 1), (0, -1))
             if s < last or (hf == 0) == (way > 0)]
    for m in moves:
        if m[0] == 0:
            ring_copy(*m).start()

    for d in order:
        wc_copy(d).wait_recv()
        wz_copy(d).wait_recv()
    wown_cp.wait()
    res_cp.wait()

    acc[...] = res[...].astype(F32) + dot(gath[y], wcol[y])
    for s in range(last + 1):
        for m in moves:
            if m[0] == s:
                ring_copy(*m).wait_recv()
                nxt = (s + 1, m[1], m[2])
                if nxt in moves:
                    ring_copy(*nxt).start()
        right = lax.rem(y + ring - s - 1, ring)
        left = lax.rem(y + s + 1, ring)
        if s < last:
            acc[...] += dot(gath[right], wcol[right]) + dot(gath[left], wcol[left])
        else:
            out_ref[...] = (acc[...] + dot(gath[right], wcol[right])).astype(BF16)

    whole(ids_s, ids_r, ids_ss, ids_rs).wait_send()
    whole(send, recv, dat_ss, dat_rs).wait_send()
    whole(rsend, rrecv, ret_ss, ret_rs).wait_send()
    for d in order:
        wy_copy(d).wait_send()
        wc_copy(d).wait_send()
        wx_copy(d).wait_send()
        wz_copy(d).wait_send()
    for m in moves:
        ring_copy(*m).wait_send()


def body(groups, ring, residual, fresh_qkv, active, home_slot, kv_cache, lengths, w_out):
    n = home_slot.shape[0]
    width = fresh_qkv.shape[2]
    cols = residual.shape[1]
    depth = w_out.shape[0]
    length = kv_cache.shape[2]
    hbm = pl.BlockSpec(memory_space=pl.ANY)
    vm = pl.BlockSpec(memory_space=pltpu.VMEM)
    dma = pltpu.SemaphoreType.DMA
    return pl.pallas_call(
        functools.partial(kernel, groups, ring),
        out_shape=jax.ShapeDtypeStruct((n, cols), BF16),
        in_specs=[hbm, vm, vm, vm, hbm, hbm, hbm],
        out_specs=vm,
        scratch_shapes=[
            pltpu.VMEM((3, n, width), BF16),
            pltpu.VMEM(kv_cache.shape, BF16),
            pltpu.VMEM((ring, depth, cols), BF16),
            pltpu.VMEM((n, cols), BF16),
            pltpu.VMEM((groups, 1, 128), F32),
            pltpu.VMEM((groups, 1, 128), F32),
            pltpu.VMEM((groups, 8, 3 * HD), BF16),
            pltpu.VMEM((groups, 8, 3 * HD), BF16),
            pltpu.VMEM((groups, 8, HD), BF16),
            pltpu.VMEM((groups, 8, HD), BF16),
            pltpu.VMEM((ring, n, width), BF16),
            pltpu.VMEM((2, groups * 8, n), BF16),
            pltpu.VMEM((2, n, groups * 8), BF16),
            pltpu.VMEM((2, n, 3 * HD), BF16),
            pltpu.VMEM((n, 16 * length), F32),
            pltpu.VMEM((2, n, HD), BF16),
            pltpu.VMEM((n, cols), F32),
            dma((7,)),
            dma, dma, dma, dma, dma, dma,
            dma((ring,)), dma((ring,)), dma((ring,)), dma((ring,)),
            dma((ring,)), dma((ring,)), dma((ring,)), dma((ring,)),
            dma((ring,)), dma((ring,)), dma((ring,)), dma((ring,)),
        ],
        compiler_params=pltpu.CompilerParams(collective_id=0, has_side_effects=True),
    )(
        fresh_qkv.transpose(1, 0, 2), active.reshape(1, n), home_slot.reshape(1, n), lengths.reshape(1, n),
        kv_cache, w_out, residual,
    )


def solution(mesh):
    placed = (
        P("dp", "tensor"),
        P("dp", None, "tensor"),
        P("dp"),
        P("dp"),
        P("dp", None, None, "tensor"),
        P("dp"),
        P("tensor", None),
    )
    return jax.shard_map(
        functools.partial(body, mesh.shape["dp"], mesh.shape["tensor"]),
        mesh=mesh, in_specs=placed, out_specs=P("dp", "tensor"), check_vma=False,
    )
```

```python
import functools

import jax
import jax.numpy as jnp
from jax import lax
from jax.experimental import pallas as pl
from jax.experimental.pallas import tpu as pltpu
from jax.sharding import PartitionSpec as P

MESH = pl.DeviceIdType.MESH
HD = 128
CAP = 4
F32, BF16, I32 = jnp.float32, jnp.bfloat16, jnp.int32


def dot(a, b, ca=1, cb=0):
    return lax.dot_general(a, b, (((ca,), (cb,)), ((), ())), preferred_element_type=F32)


def kernel(
    groups, ring,
    fresh_hbm, act_hbm, home_hbm, len_hbm, kv_hbm, w_hbm, res_hbm,
    out_ref,
    fresh, act_ref, home_ref, len_ref, kv, wcol, res, ids_s, ids_r, send, recv, rsend, rrecv, lse_s, lse_r,
    gath, place, match, owned, score, att, own_sc, live, acc,
    lsem, ids_ss, ids_rs, dat_ss, dat_rs, lse_ss, lse_rs, ret_ss, ret_rs, wy_s, wy_r, wm_s, wm_r, ag_s, ag_r,
):
    n = act_ref.shape[1]
    length = kv.shape[2]
    cols = wcol.shape[2]
    depth = wcol.shape[1]
    planes = groups // 8
    me = lax.axis_index("dp")
    y = lax.axis_index("tensor")
    z, x, core = me // 8, lax.rem(me, 8) // 2, lax.rem(me, 2)
    partner = me + 1 - 2 * core

    beside = [lax.rem(me + m, 8) for m in range(8)]

    def each_peer(act):
        def plane(i, c):
            dz = planes // 2 + (1 - 2 * lax.rem(i, 2)) * ((i + 1) // 2)
            base = lax.rem(z + dz, planes) * 8
            for m in range(8):
                act(base + beside[7 - m])
            return c

        lax.fori_loop(0, planes - 1, plane, 0)
        for m in range(7):
            act(z * 8 + beside[7 - m])

    def y_peer(d):
        return lax.rem(y + d, ring)

    barrier = pltpu.get_barrier_semaphore()

    def greet(to):
        pl.semaphore_signal(barrier, inc=1, device_id={"dp": to}, device_id_type=MESH)

    small = [pltpu.make_async_copy(a, b, lsem.at[i]) for i, (a, b) in enumerate(
        ((home_hbm, home_ref), (act_hbm, act_ref), (len_hbm, len_ref)))]
    for cp in small:
        cp.start()
    fresh_cp = pltpu.make_async_copy(fresh_hbm, fresh, lsem.at[3])
    fresh_cp.start()
    each_peer(greet)
    for d in range(1, ring):
        pl.semaphore_signal(barrier, inc=1, device_id={"tensor": y_peer(d)}, device_id_type=MESH)
    kv_cp = pltpu.make_async_copy(kv_hbm, kv, lsem.at[4])
    kv_cp.start()
    wown_cp = pltpu.make_async_copy(
        w_hbm.at[:, pl.ds(pl.multiple_of(y * cols, cols), cols)], wcol.at[ring - 1], lsem.at[5])
    wown_cp.start()
    res_cp = pltpu.make_async_copy(res_hbm, res, lsem.at[6])
    res_cp.start()

    for cp in small:
        cp.wait()
    home = home_ref[...]
    active = act_ref[...] > 0
    owner = home // n
    local_id = (home - owner * n + 1).astype(F32)
    of_group = (owner == lax.broadcasted_iota(I32, (groups, n), 0)) & active
    one_hot = jnp.where(of_group, 1.0, 0.0).astype(F32)
    before = jnp.where(
        lax.broadcasted_iota(I32, (n, n), 0) < lax.broadcasted_iota(I32, (n, n), 1), 1.0, 0.0
    ).astype(BF16)
    earlier = dot(one_hot.astype(BF16), before)
    rank = jnp.sum(one_hot * earlier, axis=0, keepdims=True)
    lane = lax.broadcasted_iota(I32, (groups, 128), 1)
    mine = (lane // 8) == lax.rem(me, 16)
    id_rows = jnp.zeros((groups, 128), F32)
    for r in range(CAP):
        value = jnp.sum(jnp.where(rank == r, one_hot * local_id, 0.0), axis=1, keepdims=True)
        id_rows = jnp.where(mine & (lane % 4 == r), value, id_rows)
    ids_s[...] = id_rows.reshape(groups, 1, 128)
    target = jnp.where(active, owner * 8 + rank.astype(I32), -64)
    spot = lax.broadcasted_iota(I32, (groups * 8, n), 0)
    fresh_cp.wait()
    rows = jnp.zeros((groups * 8, HD), F32)
    for h in range(2):
        rows += dot(jnp.where(spot == target + 4 * h, 1.0, 0.0).astype(BF16), fresh[0, :, h * HD:(h + 1) * HD])
    send[...] = rows.astype(BF16).reshape(groups, 8, HD)

    pl.semaphore_wait(barrier, groups - 1 + ring - 1)

    piece = depth // 8
    order = [1, 7, 2, 6, 3, 5, 4]
    parts = ((0, 4), (4, 3))

    def piece_of(dx):
        return (lax.rem(x + dx + 4, 4) * 2 + core) * piece

    def wy_copy(p):
        to = y_peer(order[p])
        rows = pl.ds(pl.multiple_of(piece_of(0), piece), piece)
        return pltpu.make_async_remote_copy(
            w_hbm.at[rows, pl.ds(pl.multiple_of(to * cols, cols), cols)], wcol.at[p, rows],
            wy_s.at[p], wy_r.at[p], device_id={"tensor": to}, device_id_type=MESH)

    def wmove(kind, g):
        to_x = lambda dx: z * 8 + lax.rem(x + dx + 4, 4) * 2 + core
        dx, start, size, to = (
            (0, 0, piece, to_x(1)), (0, 0, piece, to_x(-1)),
            (-1, 0, piece // 2, to_x(1)), (1, piece // 2, piece // 2, to_x(-1)),
            (0, 0, piece, partner), (-1, 0, piece, partner), (1, 0, piece, partner), (2, 0, piece, partner),
        )[kind]
        at = wcol.at[pl.ds(*parts[g]), pl.ds(pl.multiple_of(piece_of(dx) + start, size), size)]
        return pltpu.make_async_remote_copy(
            at, at, wm_s.at[2 * kind + g], wm_r.at[2 * kind + g], device_id={"dp": to}, device_id_type=MESH)

    def pass_own(g):
        for p in range(parts[g][0], sum(parts[g])):
            wy_copy(p).wait_recv()
        for kind in (0, 1, 4):
            wmove(kind, g).start()

    def pass_sides(g):
        for side in (0, 1):
            wmove(side, g).wait_recv()
            wmove(2 + side, g).start()
            wmove(5 + side, g).start()

    def pass_last(g):
        wmove(2, g).wait_recv()
        wmove(3, g).wait_recv()
        wmove(7, g).start()

    def to_peer(src, dst, ss, rs, to):
        return pltpu.make_async_remote_copy(
            src.at[to], dst.at[me], ss, rs, device_id={"dp": to}, device_id_type=MESH)

    def whole(src, dst, ss, rs):
        return pltpu.make_async_remote_copy(
            src.at[pl.ds(0, groups - 1)], dst.at[pl.ds(0, groups - 1)], ss, rs,
            device_id={"dp": partner}, device_id_type=MESH)

    ids_x = (ids_s, ids_r, ids_ss, ids_rs)
    dat_x = (send, recv, dat_ss, dat_rs)
    lse_x = (lse_s, lse_r, lse_ss, lse_rs)
    ret_x = (rsend, rrecv, ret_ss, ret_rs)

    def go(to):
        to_peer(*ids_x, to).start()
        to_peer(*dat_x, to).start()

    for p in range(ring - 1):
        wy_copy(p).start()
    each_peer(go)
    keep = [pltpu.make_async_copy(a.at[me], b.at[me], lsem.at[7 + i]) for i, (a, b) in enumerate(
        ((ids_s, ids_r), (send, recv), (lse_s, lse_r), (rsend, rrecv)))]
    keep[0].start()
    keep[1].start()

    eye = lax.broadcasted_iota(I32, (n, n), 0) == lax.broadcasted_iota(I32, (n, n), 1)

    def as_column(row, wide):
        return dot(jnp.where(eye, row, 0).astype(BF16), jnp.ones((n, wide), BF16))

    lengths = as_column(len_ref[...].astype(F32), 16 * length)
    spot_col = (as_column(jnp.where(active, owner, -8).astype(F32), groups * 8) * 8
                + as_column(rank, groups * 8)).astype(I32)
    live[...] = jnp.where(spot_col[:, 0:HD] >= 0, 1.0, 0.0)
    spot_row = lax.broadcasted_iota(I32, (n, groups * 8), 1)
    scale = HD ** -0.5
    for h in range(2):
        cl = pl.ds(h * HD, HD)
        place[h] = jnp.where(spot_row == spot_col + 4 * h, 1.0, 0.0).astype(BF16)
        own = jnp.sum(fresh[0, :, cl].astype(F32) * fresh[1, :, cl].astype(F32), axis=1, keepdims=True) * scale
        own_sc[h] = jnp.broadcast_to(own, (n, HD))

    keep[0].wait()
    whole(*ids_x).wait_recv()

    def lanes_of(ref, b):
        total = ref[16 * b]
        for i in range(1, 16):
            total = total + ref[16 * b + i]
        return total

    slot = lax.broadcasted_iota(I32, (n, 128), 0) + 1
    half = (lax.broadcasted_iota(I32, (n, 128), 1) % 8) // 4
    for b in range(groups // 16):
        hit = lanes_of(ids_r, b).astype(I32) == slot
        for h in range(2):
            match[h, :, b * 128:(b + 1) * 128] = jnp.where(hit & (half == h), 1.0, 0.0).astype(BF16)
    keep[1].wait()
    whole(*dat_x).wait_recv()
    arrived = recv[...].reshape(groups * 8, HD)
    for h in range(2):
        owned[h] = dot(match[h], arrived).astype(BF16)

    kv_cp.wait()
    blocks = n // 16
    lane_i = lax.broadcasted_iota(I32, (n, 16 * length), 1)
    row_i = lax.broadcasted_iota(I32, (n, 16 * length), 0)
    valid = (lane_i // length == row_i % 16) & ((lane_i % length).astype(F32) < lengths)
    lse_row = jnp.zeros((1, groups * 8), F32)
    for h in range(2):
        cl = pl.ds(h * HD, HD)
        for i in range(blocks):
            keys = kv[16 * i:16 * i + 16, 0, :, cl].reshape(16 * length, HD)
            score[16 * i:16 * i + 16] = dot(owned[h, 16 * i:16 * i + 16], keys, 1, 1)
        s = jnp.where(valid, score[...] * scale, -1e30)
        top = jnp.max(s, axis=1, keepdims=True)
        e = jnp.where(valid, jnp.exp(s - top), 0.0)
        total = jnp.sum(e, axis=1, keepdims=True)
        w = (e / total).astype(BF16)
        lse_row += jnp.sum(match[h].astype(F32) * (top + jnp.log(total)), axis=0, keepdims=True)
        for i in range(blocks):
            values = kv[16 * i:16 * i + 16, 1, :, cl].reshape(16 * length, HD)
            att[h, 16 * i:16 * i + 16] = dot(w[16 * i:16 * i + 16], values).astype(BF16)
    back = dot(match[0], att[0], 0, 0) + dot(match[1], att[1], 0, 0)
    rsend[...] = back.astype(BF16).reshape(groups, 8, HD)
    spread = jnp.zeros((groups, 128), F32)
    group_i = lax.broadcasted_iota(I32, (groups, 128), 0)
    for b in range(groups // 16):
        spread = jnp.where(group_i // 16 == b, lse_row[:, b * 128:(b + 1) * 128], spread)
    lse_rows = jnp.zeros((groups, 128), F32)
    for i in range(8):
        value = jnp.sum(jnp.where(lane == (group_i % 16) * 8 + i, spread, 0.0), axis=1, keepdims=True)
        lse_rows = jnp.where(mine & (lane % 8 == i), value, lse_rows)
    lse_s[...] = lse_rows.reshape(groups, 1, 128)

    def go_back(to):
        to_peer(*lse_x, to).start()
        to_peer(*ret_x, to).start()

    each_peer(go_back)
    keep[2].start()
    keep[3].start()

    pass_own(0)
    pass_own(1)

    keep[2].wait()
    whole(*lse_x).wait_recv()
    lse_got = [lanes_of(lse_r, b) for b in range(groups // 16)]
    keep[3].wait()
    whole(*ret_x).wait_recv()
    back_rows = rrecv[...].reshape(groups * 8, HD)
    for h in range(2):
        cl = pl.ds(h * HD, HD)
        cached = dot(place[h], back_rows)
        lse = jnp.zeros((n, 128), F32)
        for b in range(groups // 16):
            lse += place[h, :, b * 128:(b + 1) * 128].astype(F32) * lse_got[b]
        lse = jnp.sum(lse, axis=1, keepdims=True)
        own = own_sc[h]
        top = jnp.maximum(lse, own)
        of_cache, of_own = jnp.exp(lse - top), jnp.exp(own - top)
        mixed = (of_cache * cached + of_own * fresh[2, :, cl].astype(F32)) / (of_cache + of_own)
        gath[y, :, cl] = (mixed * live[...]).astype(BF16)

    pieces = 4
    hr = n // pieces

    def ring_copy(s, q, way):
        src = lax.rem(y + (ring - s if way > 0 else s), ring)
        to = lax.rem(y + (1 if way > 0 else ring - 1), ring)
        at = gath.at[src, pl.ds(q * hr, hr)]
        i = (s * pieces + q) * 2 + (way > 0)
        return pltpu.make_async_remote_copy(
            at, at, ag_s.at[i], ag_r.at[i], device_id={"tensor": to}, device_id_type=MESH)

    last = ring // 2 - 1
    moves = [(s, q if way > 0 else pieces - 1 - q, way)
             for s in range(last + 1) for q in range(pieces) for way in (1, -1)
             if s < last or q < pieces // 2]
    for m in moves:
        if m[0] == 0:
            ring_copy(*m).start()

    pass_sides(0)
    pass_sides(1)

    def relay(s):
        for m in moves:
            if m[0] == s:
                ring_copy(*m).wait_recv()
                nxt = (s + 1, m[1], m[2])
                if nxt in moves:
                    ring_copy(*nxt).start()

    def project(d):
        return dot(gath[lax.rem(y + ring - d, ring)], wcol[order.index(d)])

    relay(0)
    pass_last(0)
    pass_last(1)
    wown_cp.wait()
    res_cp.wait()
    acc[...] = res[...].astype(F32) + dot(gath[y], wcol[ring - 1])
    relay(1)
    for g in range(2):
        for kind in range(4, 8):
            wmove(kind, g).wait_recv()
    acc[...] += project(1) + project(ring - 1)
    relay(2)
    acc[...] += project(2) + project(ring - 2)
    acc[...] += project(3) + project(ring - 3)
    relay(3)
    out_ref[...] = (acc[...] + project(4)).astype(BF16)

    for ex in (ids_x, dat_x, lse_x, ret_x):
        whole(*ex).wait_send()
    for p in range(ring - 1):
        wy_copy(p).wait_send()
    for g in range(2):
        for kind in range(8):
            wmove(kind, g).wait_send()
    for m in moves:
        ring_copy(*m).wait_send()


def body(groups, ring, residual, fresh_qkv, active, home_slot, kv_cache, lengths, w_out):
    n = home_slot.shape[0]
    width = fresh_qkv.shape[2]
    cols = residual.shape[1]
    depth = w_out.shape[0]
    length = kv_cache.shape[2]
    hbm = pl.BlockSpec(memory_space=pl.ANY)
    dma = pltpu.SemaphoreType.DMA
    return pl.pallas_call(
        functools.partial(kernel, groups, ring),
        out_shape=jax.ShapeDtypeStruct((n, cols), BF16),
        in_specs=[hbm] * 7,
        out_specs=pl.BlockSpec(memory_space=pltpu.VMEM),
        scratch_shapes=[
            pltpu.VMEM((3, n, width), BF16),
            pltpu.VMEM((1, n), I32),
            pltpu.VMEM((1, n), I32),
            pltpu.VMEM((1, n), I32),
            pltpu.VMEM(kv_cache.shape, BF16),
            pltpu.VMEM((ring, depth, cols), BF16),
            pltpu.VMEM((n, cols), BF16),
            pltpu.VMEM((groups, 1, 128), F32),
            pltpu.VMEM((groups, 1, 128), F32),
            pltpu.VMEM((groups, 8, HD), BF16),
            pltpu.VMEM((groups, 8, HD), BF16),
            pltpu.VMEM((groups, 8, HD), BF16),
            pltpu.VMEM((groups, 8, HD), BF16),
            pltpu.VMEM((groups, 1, 128), F32),
            pltpu.VMEM((groups, 1, 128), F32),
            pltpu.VMEM((ring, n, width), BF16),
            pltpu.VMEM((2, n, groups * 8), BF16),
            pltpu.VMEM((2, n, groups * 8), BF16),
            pltpu.VMEM((2, n, HD), BF16),
            pltpu.VMEM((n, 16 * length), F32),
            pltpu.VMEM((2, n, HD), BF16),
            pltpu.VMEM((2, n, HD), F32),
            pltpu.VMEM((n, HD), F32),
            pltpu.VMEM((n, cols), F32),
            dma((11,)),
            dma, dma, dma, dma, dma, dma, dma, dma,
            dma((ring,)), dma((ring,)), dma((16,)), dma((16,)), dma((32,)), dma((32,)),
        ],
        compiler_params=pltpu.CompilerParams(collective_id=0, has_side_effects=True),
    )(
        fresh_qkv.transpose(1, 0, 2), active.reshape(1, n), home_slot.reshape(1, n), lengths.reshape(1, n),
        kv_cache, w_out, residual,
    )


def solution(mesh):
    placed = (
        P("dp", "tensor"),
        P("dp", None, "tensor"),
        P("dp"),
        P("dp"),
        P("dp", None, None, "tensor"),
        P("dp"),
        P("tensor", None),
    )
    return jax.shard_map(
        functools.partial(body, mesh.shape["dp"], mesh.shape["tensor"]),
        mesh=mesh, in_specs=placed, out_specs=P("dp", "tensor"), check_vma=False,
    )
```

```python
import functools

import jax
import jax.numpy as jnp
from jax import lax
from jax.experimental import pallas as pl
from jax.experimental.pallas import tpu as pltpu
from jax.sharding import PartitionSpec as P

MESH = pl.DeviceIdType.MESH
HD = 128
CAP = 4
F32, BF16, I32 = jnp.float32, jnp.bfloat16, jnp.int32


def dot(a, b, ca=1, cb=0):
    return lax.dot_general(a, b, (((ca,), (cb,)), ((), ())), preferred_element_type=F32)


def kernel(
    groups, ring,
    fresh_hbm, act_hbm, home_hbm, len_hbm, kv_hbm, w_hbm, res_hbm,
    out_ref,
    fresh, small, kv, wcol, res, ids_s, ids_r, send, recv, rsend, rrecv, lse_s, lse_r,
    gath, place, match, owned, score, att, own_sc, live, acc,
    lsem, ids_ss, ids_rs, dat_ss, dat_rs, lse_ss, lse_rs, ret_ss, ret_rs, w_sem, wy_r, wm_r, ag_s, ag_r,
):
    n = small.shape[2]
    length = kv.shape[2]
    cols = wcol.shape[2]
    depth = wcol.shape[1]
    planes = groups // 8
    me = lax.axis_index("dp")
    y = lax.axis_index("tensor")
    z, x, core = me // 8, lax.rem(me, 8) // 2, lax.rem(me, 2)
    partner = me + 1 - 2 * core

    beside = [lax.rem(me + m, 8) for m in range(8)]

    def each_peer(act):
        def plane(i, c):
            dz = planes // 2 + (1 - 2 * lax.rem(i, 2)) * ((i + 1) // 2)
            base = lax.rem(z + dz, planes) * 8
            for m in range(8):
                act(base + beside[7 - m])
            return c

        lax.fori_loop(0, planes - 1, plane, 0)
        for m in range(7):
            act(z * 8 + beside[7 - m])

    def y_peer(d):
        return lax.rem(y + d, ring)

    barrier = pltpu.get_barrier_semaphore()

    def greet(to):
        pl.semaphore_signal(barrier, inc=1, device_id={"dp": to}, device_id_type=MESH)

    for i, a in enumerate((home_hbm, act_hbm, len_hbm)):
        pltpu.make_async_copy(a, small.at[i], lsem.at[0]).start()
    fresh_cp = pltpu.make_async_copy(fresh_hbm, fresh, lsem.at[1])
    fresh_cp.start()
    each_peer(greet)
    for d in range(1, ring):
        pl.semaphore_signal(barrier, inc=1, device_id={"tensor": y_peer(d)}, device_id_type=MESH)
    kv_cp = pltpu.make_async_copy(kv_hbm, kv, lsem.at[2])
    kv_cp.start()
    wown_cp = pltpu.make_async_copy(
        w_hbm.at[:, pl.ds(pl.multiple_of(y * cols, cols), cols)], wcol.at[ring - 1], lsem.at[3])
    wown_cp.start()
    res_cp = pltpu.make_async_copy(res_hbm, res, lsem.at[4])
    res_cp.start()

    pltpu.make_async_copy(small, small, lsem.at[0]).wait()
    home = small[0]
    active = small[1] > 0
    owner = home // n
    local_id = (home - owner * n + 1).astype(F32)
    of_group = (owner == lax.broadcasted_iota(I32, (groups, n), 0)) & active
    one_hot = jnp.where(of_group, 1.0, 0.0).astype(F32)
    before = jnp.where(
        lax.broadcasted_iota(I32, (n, n), 0) < lax.broadcasted_iota(I32, (n, n), 1), 1.0, 0.0
    ).astype(BF16)
    earlier = dot(one_hot.astype(BF16), before)
    rank = jnp.sum(one_hot * earlier, axis=0, keepdims=True)
    lane = lax.broadcasted_iota(I32, (groups, 128), 1)
    mine = (lane // 8) == lax.rem(me, 16)
    id_rows = jnp.zeros((groups, 128), F32)
    for r in range(CAP):
        value = jnp.sum(jnp.where(rank == r, one_hot * local_id, 0.0), axis=1, keepdims=True)
        id_rows = jnp.where(mine & (lane % 4 == r), value, id_rows)
    ids_s[...] = id_rows.reshape(groups, 1, 128)
    target = jnp.where(active, owner * 8 + rank.astype(I32), -64)
    spot = lax.broadcasted_iota(I32, (groups * 8, n), 0)
    fresh_cp.wait()
    rows = jnp.zeros((groups * 8, HD), F32)
    for h in range(2):
        rows += dot(jnp.where(spot == target + 4 * h, 1.0, 0.0).astype(BF16), fresh[0, :, h * HD:(h + 1) * HD])
    send[...] = rows.astype(BF16).reshape(groups, 8, HD)

    pl.semaphore_wait(barrier, groups - 1 + ring - 1)

    piece = depth // 8
    order = [1, 7, 2, 6, 3, 5, 4]
    parts = ((0, 4), (4, 3))

    def piece_of(dx):
        return (lax.rem(x + dx + 4, 4) * 2 + core) * piece

    def wy_copy(p):
        to = y_peer(order[p])
        rows = pl.ds(pl.multiple_of(piece_of(0), piece), piece)
        return pltpu.make_async_remote_copy(
            w_hbm.at[rows, pl.ds(pl.multiple_of(to * cols, cols), cols)], wcol.at[p, rows],
            w_sem, wy_r.at[int(p >= parts[1][0])], device_id={"tensor": to}, device_id_type=MESH)

    def wmove(kind, g):
        slot_of = (0, 2, 4, 4, 6, 6, 6, 6)
        to_x = lambda dx: z * 8 + lax.rem(x + dx + 4, 4) * 2 + core
        dx, start, size, to = (
            (0, 0, piece, to_x(1)), (0, 0, piece, to_x(-1)),
            (-1, 0, piece // 2, to_x(1)), (1, piece // 2, piece // 2, to_x(-1)),
            (0, 0, piece, partner), (-1, 0, piece, partner), (1, 0, piece, partner), (2, 0, piece, partner),
        )[kind]
        at = wcol.at[pl.ds(*parts[g]), pl.ds(pl.multiple_of(piece_of(dx) + start, size), size)]
        return pltpu.make_async_remote_copy(
            at, at, w_sem, wm_r.at[slot_of[kind] + (g if kind < 4 else 0)], device_id={"dp": to}, device_id_type=MESH)

    def w_all(recv_sem, rows, first, count):
        at = wcol.at[pl.ds(first, count), pl.ds(0, rows)]
        return pltpu.make_async_remote_copy(
            at, at, w_sem, recv_sem, device_id={"dp": partner}, device_id_type=MESH)

    def pass_own(g):
        w_all(wy_r.at[g], piece, *parts[g]).wait_recv()
        for kind in (0, 1, 4):
            wmove(kind, g).start()

    def pass_sides(g):
        for side in (0, 1):
            wmove(side, g).wait_recv()
            wmove(2 + side, g).start()
            wmove(5 + side, g).start()

    def pass_last(g):
        w_all(wm_r.at[4 + g], piece, *parts[g]).wait_recv()
        wmove(7, g).start()

    def to_peer(src, dst, ss, rs, to):
        return pltpu.make_async_remote_copy(
            src.at[to], dst.at[me], ss, rs, device_id={"dp": to}, device_id_type=MESH)

    def whole(src, dst, ss, rs):
        return pltpu.make_async_remote_copy(
            src.at[pl.ds(0, groups - 1)], dst.at[pl.ds(0, groups - 1)], ss, rs,
            device_id={"dp": partner}, device_id_type=MESH)

    ids_x = (ids_s, ids_r, ids_ss, ids_rs)
    dat_x = (send, recv, dat_ss, dat_rs)
    lse_x = (lse_s, lse_r, lse_ss, lse_rs)
    ret_x = (rsend, rrecv, ret_ss, ret_rs)

    def go(to):
        to_peer(*ids_x, to).start()
        to_peer(*dat_x, to).start()

    for p in range(ring - 1):
        wy_copy(p).start()
    each_peer(go)
    keep = [pltpu.make_async_copy(a.at[me], b.at[me], lsem.at[5 + i]) for i, (a, b) in enumerate(
        ((ids_s, ids_r), (send, recv), (lse_s, lse_r), (rsend, rrecv)))]
    keep[0].start()
    keep[1].start()

    eye = lax.broadcasted_iota(I32, (n, n), 0) == lax.broadcasted_iota(I32, (n, n), 1)

    def as_column(row, wide):
        return dot(jnp.where(eye, row, 0).astype(BF16), jnp.ones((n, wide), BF16))

    lengths = as_column(small[2].astype(F32), 16 * length)
    spot_col = (as_column(jnp.where(active, owner, -8).astype(F32), groups * 8) * 8
                + as_column(rank, groups * 8)).astype(I32)
    live[...] = jnp.where(spot_col[:, 0:HD] >= 0, 1.0, 0.0)
    spot_row = lax.broadcasted_iota(I32, (n, groups * 8), 1)
    scale = HD ** -0.5
    for h in range(2):
        cl = pl.ds(h * HD, HD)
        place[h] = jnp.where(spot_row == spot_col + 4 * h, 1.0, 0.0).astype(BF16)
        own = jnp.sum(fresh[0, :, cl].astype(F32) * fresh[1, :, cl].astype(F32), axis=1, keepdims=True) * scale
        own_sc[h] = jnp.broadcast_to(own, (n, HD))

    keep[0].wait()
    whole(*ids_x).wait_recv()

    def lanes_of(ref, b):
        total = ref[16 * b]
        for i in range(1, 16):
            total = total + ref[16 * b + i]
        return total

    slot = lax.broadcasted_iota(I32, (n, 128), 0) + 1
    half = (lax.broadcasted_iota(I32, (n, 128), 1) % 8) // 4
    for b in range(groups // 16):
        hit = lanes_of(ids_r, b).astype(I32) == slot
        for h in range(2):
            match[h, :, b * 128:(b + 1) * 128] = jnp.where(hit & (half == h), 1.0, 0.0).astype(BF16)
    keep[1].wait()
    whole(*dat_x).wait_recv()
    arrived = recv[...].reshape(groups * 8, HD)
    for h in range(2):
        owned[h] = dot(match[h], arrived).astype(BF16)

    kv_cp.wait()
    blocks = n // 16
    lane_i = lax.broadcasted_iota(I32, (n, 16 * length), 1)
    row_i = lax.broadcasted_iota(I32, (n, 16 * length), 0)
    valid = (lane_i // length == row_i % 16) & ((lane_i % length).astype(F32) < lengths)
    lse_row = jnp.zeros((1, groups * 8), F32)
    for h in range(2):
        cl = pl.ds(h * HD, HD)
        for i in range(blocks):
            keys = kv[16 * i:16 * i + 16, 0, :, cl].reshape(16 * length, HD)
            score[16 * i:16 * i + 16] = dot(owned[h, 16 * i:16 * i + 16], keys, 1, 1)
        s = jnp.where(valid, score[...] * scale, -1e30)
        top = jnp.max(s, axis=1, keepdims=True)
        e = jnp.where(valid, jnp.exp(s - top), 0.0)
        total = jnp.sum(e, axis=1, keepdims=True)
        w = (e / total).astype(BF16)
        lse_row += jnp.sum(match[h].astype(F32) * (top + jnp.log(total)), axis=0, keepdims=True)
        for i in range(blocks):
            values = kv[16 * i:16 * i + 16, 1, :, cl].reshape(16 * length, HD)
            att[h, 16 * i:16 * i + 16] = dot(w[16 * i:16 * i + 16], values).astype(BF16)
    back = dot(match[0], att[0], 0, 0) + dot(match[1], att[1], 0, 0)
    rsend[...] = back.astype(BF16).reshape(groups, 8, HD)
    spread = jnp.zeros((groups, 128), F32)
    group_i = lax.broadcasted_iota(I32, (groups, 128), 0)
    for b in range(groups // 16):
        spread = jnp.where(group_i // 16 == b, lse_row[:, b * 128:(b + 1) * 128], spread)
    lse_rows = jnp.zeros((groups, 128), F32)
    for i in range(8):
        value = jnp.sum(jnp.where(lane == (group_i % 16) * 8 + i, spread, 0.0), axis=1, keepdims=True)
        lse_rows = jnp.where(mine & (lane % 8 == i), value, lse_rows)
    lse_s[...] = lse_rows.reshape(groups, 1, 128)

    def go_back(to):
        to_peer(*lse_x, to).start()
        to_peer(*ret_x, to).start()

    each_peer(go_back)
    keep[2].start()
    keep[3].start()

    pass_own(0)
    pass_own(1)

    keep[2].wait()
    whole(*lse_x).wait_recv()
    lse_got = [lanes_of(lse_r, b) for b in range(groups // 16)]
    keep[3].wait()
    whole(*ret_x).wait_recv()
    back_rows = rrecv[...].reshape(groups * 8, HD)
    for h in range(2):
        cl = pl.ds(h * HD, HD)
        cached = dot(place[h], back_rows)
        lse = jnp.zeros((n, 128), F32)
        for b in range(groups // 16):
            lse += place[h, :, b * 128:(b + 1) * 128].astype(F32) * lse_got[b]
        lse = jnp.sum(lse, axis=1, keepdims=True)
        own = own_sc[h]
        top = jnp.maximum(lse, own)
        of_cache, of_own = jnp.exp(lse - top), jnp.exp(own - top)
        mixed = (of_cache * cached + of_own * fresh[2, :, cl].astype(F32)) / (of_cache + of_own)
        gath[y, :, cl] = (mixed * live[...]).astype(BF16)

    pieces = 4
    hr = n // pieces

    def ring_copy(s, q, way):
        src = lax.rem(y + (ring - s if way > 0 else s), ring)
        to = lax.rem(y + (1 if way > 0 else ring - 1), ring)
        at = gath.at[src, pl.ds(q * hr, hr)]
        i = (s * pieces + q) * 2 + (way > 0)
        return pltpu.make_async_remote_copy(
            at, at, ag_s, ag_r.at[i], device_id={"tensor": to}, device_id_type=MESH)

    last = ring // 2 - 1
    moves = [(s, q if way > 0 else pieces - 1 - q, way)
             for s in range(last + 1) for q in range(pieces) for way in (1, -1)
             if s < last or q < pieces // 2]
    for m in moves:
        if m[0] == 0:
            ring_copy(*m).start()

    pass_sides(0)
    pass_sides(1)

    def relay(s):
        for m in moves:
            if m[0] == s:
                ring_copy(*m).wait_recv()
                nxt = (s + 1, m[1], m[2])
                if nxt in moves:
                    ring_copy(*nxt).start()

    def project(d):
        return dot(gath[lax.rem(y + ring - d, ring)], wcol[order.index(d)])

    relay(0)
    pass_last(0)
    pass_last(1)
    wown_cp.wait()
    res_cp.wait()
    acc[...] = res[...].astype(F32) + dot(gath[y], wcol[ring - 1])
    relay(1)
    w_all(wm_r.at[6], depth // 2, 0, ring - 1).wait_recv()
    acc[...] += project(1) + project(ring - 1)
    relay(2)
    acc[...] += project(2) + project(ring - 2)
    acc[...] += project(3) + project(ring - 3)
    relay(3)
    out_ref[...] = (acc[...] + project(4)).astype(BF16)

    for ex in (ids_x, dat_x, lse_x, ret_x):
        whole(*ex).wait_send()
    w_all(wm_r.at[6], depth, 0, ring - 1).wait_send()
    ring_all = gath.at[pl.ds(0, ring - 1)]
    pltpu.make_async_remote_copy(
        ring_all, ring_all, ag_s, ag_r.at[0], device_id={"tensor": y_peer(1)}, device_id_type=MESH).wait_send()


def body(groups, ring, residual, fresh_qkv, active, home_slot, kv_cache, lengths, w_out):
    n = home_slot.shape[0]
    width = fresh_qkv.shape[2]
    cols = residual.shape[1]
    depth = w_out.shape[0]
    length = kv_cache.shape[2]
    hbm = pl.BlockSpec(memory_space=pl.ANY)
    dma = pltpu.SemaphoreType.DMA
    return pl.pallas_call(
        functools.partial(kernel, groups, ring),
        out_shape=jax.ShapeDtypeStruct((n, cols), BF16),
        in_specs=[hbm] * 7,
        out_specs=pl.BlockSpec(memory_space=pltpu.VMEM),
        scratch_shapes=[
            pltpu.VMEM((3, n, width), BF16),
            pltpu.VMEM((3, 1, n), I32),
            pltpu.VMEM(kv_cache.shape, BF16),
            pltpu.VMEM((ring, depth, cols), BF16),
            pltpu.VMEM((n, cols), BF16),
            pltpu.VMEM((groups, 1, 128), F32),
            pltpu.VMEM((groups, 1, 128), F32),
            pltpu.VMEM((groups, 8, HD), BF16),
            pltpu.VMEM((groups, 8, HD), BF16),
            pltpu.VMEM((groups, 8, HD), BF16),
            pltpu.VMEM((groups, 8, HD), BF16),
            pltpu.VMEM((groups, 1, 128), F32),
            pltpu.VMEM((groups, 1, 128), F32),
            pltpu.VMEM((ring, n, width), BF16),
            pltpu.VMEM((2, n, groups * 8), BF16),
            pltpu.VMEM((2, n, groups * 8), BF16),
            pltpu.VMEM((2, n, HD), BF16),
            pltpu.VMEM((n, 16 * length), F32),
            pltpu.VMEM((2, n, HD), BF16),
            pltpu.VMEM((2, n, HD), F32),
            pltpu.VMEM((n, HD), F32),
            pltpu.VMEM((n, cols), F32),
            dma((9,)),
            dma, dma, dma, dma, dma, dma, dma, dma,
            dma, dma((2,)), dma((7,)), dma, dma((32,)),
        ],
        compiler_params=pltpu.CompilerParams(collective_id=0, has_side_effects=True),
    )(
        fresh_qkv.transpose(1, 0, 2), active.reshape(1, n), home_slot.reshape(1, n), lengths.reshape(1, n),
        kv_cache, w_out, residual,
    )


def solution(mesh):
    placed = (
        P("dp", "tensor"),
        P("dp", None, "tensor"),
        P("dp"),
        P("dp"),
        P("dp", None, None, "tensor"),
        P("dp"),
        P("tensor", None),
    )
    return jax.shard_map(
        functools.partial(body, mesh.shape["dp"], mesh.shape["tensor"]),
        mesh=mesh, in_specs=placed, out_specs=P("dp", "tensor"), check_vma=False,
    )
```

```python
import functools

import jax
import jax.numpy as jnp
from jax import lax
from jax.experimental import pallas as pl
from jax.experimental.pallas import tpu as pltpu
from jax.sharding import PartitionSpec as P

MESH = pl.DeviceIdType.MESH
HD = 128
CAP = 4
F32, BF16, I32 = jnp.float32, jnp.bfloat16, jnp.int32


def dot(a, b, ca=1, cb=0):
    return lax.dot_general(a, b, (((ca,), (cb,)), ((), ())), preferred_element_type=F32)


def kernel(
    groups, ring,
    fresh_hbm, act_hbm, home_hbm, len_hbm, kv_hbm, w_hbm, res_hbm,
    out_ref,
    fresh, small, kv, wcol, res, send, recv, rsend, rrecv,
    gath, place, match, owned, score, att, own_sc, live, of_owner, of_row, acc, done,
    lsem, dat_ss, dat_rs, ret_ss, ret_rs, w_sem, wy_r, wm_r, ag_s, ag_r,
):
    n = small.shape[2]
    length = kv.shape[2]
    cols = wcol.shape[2]
    depth = wcol.shape[1]
    planes = groups // 8
    me = lax.axis_index("dp")
    y = lax.axis_index("tensor")
    z, x, core = me // 8, lax.rem(me, 8) // 2, lax.rem(me, 2)
    partner = me + 1 - 2 * core

    plane_at = [lax.rem(z + dz, planes) * 8 for dz in range(planes)]
    chip_at = [lax.rem(x + dx, 4) * 2 for dx in range(4)]
    hops = lambda dz, dx: min(dz, planes - dz) + min(dx, 4 - dx)
    far_first = sorted(
        ((dz, dx) for dz in range(planes) for dx in range(4)),
        key=lambda p: (-hops(*p), abs(p[0] - planes // 2)))

    def each_peer(act):
        for dz, dx in far_first[:-1]:
            for c in range(2):
                act(plane_at[dz] + chip_at[dx] + c)
        act(partner)

    def y_peer(d):
        return lax.rem(y + d, ring)

    barrier = pltpu.get_barrier_semaphore()

    def greet(to):
        pl.semaphore_signal(barrier, inc=1, device_id={"dp": to}, device_id_type=MESH)

    for i, a in enumerate((home_hbm, act_hbm, len_hbm)):
        pltpu.make_async_copy(a, small.at[i], lsem.at[0]).start()
    fresh_cp = pltpu.make_async_copy(fresh_hbm, fresh, lsem.at[1])
    fresh_cp.start()
    each_peer(greet)
    for d in range(1, ring):
        pl.semaphore_signal(barrier, inc=1, device_id={"tensor": y_peer(d)}, device_id_type=MESH)
    kv_cp = pltpu.make_async_copy(kv_hbm, kv, lsem.at[2])
    kv_cp.start()
    wown_cp = pltpu.make_async_copy(
        w_hbm.at[:, pl.ds(pl.multiple_of(y * cols, cols), cols)], wcol.at[ring - 1], lsem.at[3])
    wown_cp.start()
    res_cp = pltpu.make_async_copy(res_hbm, res, lsem.at[4])
    res_cp.start()

    pltpu.make_async_copy(small, small, lsem.at[0]).wait()
    home = small[0]
    active = small[1] > 0
    owner = home // n
    local_id = (home - owner * n + 1).astype(F32)
    of_group = (owner == lax.broadcasted_iota(I32, (groups, n), 0)) & active
    one_hot = jnp.where(of_group, 1.0, 0.0).astype(F32)
    before = jnp.where(
        lax.broadcasted_iota(I32, (n, n), 0) < lax.broadcasted_iota(I32, (n, n), 1), 1.0, 0.0
    ).astype(BF16)
    earlier = dot(one_hot.astype(BF16), before)
    rank = jnp.sum(one_hot * earlier, axis=0, keepdims=True)
    lane = lax.broadcasted_iota(I32, (groups, 128), 1)
    mine = (lane // 8) == lax.rem(me, 16)
    id_rows = jnp.zeros((groups, 128), F32)
    for r in range(CAP):
        value = jnp.sum(jnp.where(rank == r, one_hot * local_id, 0.0), axis=1, keepdims=True)
        id_rows = jnp.where(mine & (lane % 4 == r), value, id_rows)
    first_row = lax.broadcasted_iota(I32, (groups, 2, 128), 1) == 0

    def fifth(rows):
        return jnp.where(first_row, jnp.broadcast_to(rows.reshape(groups, 1, 128), (groups, 2, 128)), 0.0).astype(BF16)

    send[:, 4] = fifth(id_rows)
    target = jnp.where(active, owner * 8 + rank.astype(I32), -64)
    spot = lax.broadcasted_iota(I32, (groups * 8, n), 0)
    fresh_cp.wait()
    rows = jnp.zeros((groups * 8, HD), F32)
    for h in range(2):
        rows += dot(jnp.where(spot == target + 4 * h, 1.0, 0.0).astype(BF16), fresh[0, :, h * HD:(h + 1) * HD])
    send[:, 0:4] = rows.astype(BF16).reshape(groups, 4, 2, HD)

    pl.semaphore_wait(barrier, groups - 1 + ring - 1)

    piece = depth // 8
    order = [1, 7, 2, 6, 3, 5, 4]
    parts = ((0, 4), (4, 3))

    def piece_of(dx):
        return (lax.rem(x + dx + 4, 4) * 2 + core) * piece

    def wy_copy(p):
        to = y_peer(order[p])
        rows = pl.ds(pl.multiple_of(piece_of(0), piece), piece)
        return pltpu.make_async_remote_copy(
            w_hbm.at[rows, pl.ds(pl.multiple_of(to * cols, cols), cols)], wcol.at[p, rows],
            w_sem, wy_r.at[int(p >= parts[1][0])], device_id={"tensor": to}, device_id_type=MESH)

    def wmove(kind, g):
        slot_of = (0, 2, 4, 4, 6, 6, 6, 6)
        to_x = lambda dx: z * 8 + lax.rem(x + dx + 4, 4) * 2 + core
        dx, start, size, to = (
            (0, 0, piece, to_x(1)), (0, 0, piece, to_x(-1)),
            (-1, 0, piece // 2, to_x(1)), (1, piece // 2, piece // 2, to_x(-1)),
            (0, 0, piece, partner), (-1, 0, piece, partner), (1, 0, piece, partner), (2, 0, piece, partner),
        )[kind]
        at = wcol.at[pl.ds(*parts[g]), pl.ds(pl.multiple_of(piece_of(dx) + start, size), size)]
        return pltpu.make_async_remote_copy(
            at, at, w_sem, wm_r.at[slot_of[kind] + (g if kind < 4 else 0)], device_id={"dp": to}, device_id_type=MESH)

    def w_all(recv_sem, rows, first, count):
        at = wcol.at[pl.ds(first, count), pl.ds(0, rows)]
        return pltpu.make_async_remote_copy(
            at, at, w_sem, recv_sem, device_id={"dp": partner}, device_id_type=MESH)

    def pass_own(g):
        w_all(wy_r.at[g], piece, *parts[g]).wait_recv()
        for kind in (0, 1, 4):
            wmove(kind, g).start()

    def pass_sides(g):
        for side in (0, 1):
            wmove(side, g).wait_recv()
            wmove(2 + side, g).start()
            wmove(5 + side, g).start()

    def pass_last(g):
        w_all(wm_r.at[4 + g], piece, *parts[g]).wait_recv()
        wmove(7, g).start()

    def to_peer(src, dst, ss, rs, to):
        return pltpu.make_async_remote_copy(
            src.at[to], dst.at[me], ss, rs, device_id={"dp": to}, device_id_type=MESH)

    def whole(src, dst, ss, rs):
        return pltpu.make_async_remote_copy(
            src.at[pl.ds(0, groups - 1)], dst.at[pl.ds(0, groups - 1)], ss, rs,
            device_id={"dp": partner}, device_id_type=MESH)

    dat_x = (send, recv, dat_ss, dat_rs)
    ret_x = (rsend, rrecv, ret_ss, ret_rs)

    for p in range(ring - 1):
        wy_copy(p).start()
    each_peer(lambda to: to_peer(*dat_x, to).start())
    keep = [pltpu.make_async_copy(a.at[me], b.at[me], lsem.at[5 + i]) for i, (a, b) in enumerate(
        ((send, recv), (rsend, rrecv)))]
    keep[0].start()

    eye = lax.broadcasted_iota(I32, (n, n), 0) == lax.broadcasted_iota(I32, (n, n), 1)

    def as_column(row, wide):
        return dot(jnp.where(eye, row, 0).astype(BF16), jnp.ones((n, wide), BF16))

    lengths = as_column(small[2].astype(F32), 16 * length)
    owner_col = as_column(jnp.where(active, owner, -8).astype(F32), groups * 8)
    rank_col = as_column(rank, groups * 8)
    spot_col = (owner_col * 8 + rank_col).astype(I32)
    lane_n = lax.broadcasted_iota(I32, (n, HD), 1)
    of_owner[...] = jnp.where(lane_n == owner_col[:, 0:HD].astype(I32) * 2, 1.0, 0.0).astype(BF16)
    live[...] = jnp.where(spot_col[:, 0:HD] >= 0, 1.0, 0.0)
    spot_row = lax.broadcasted_iota(I32, (n, groups * 8), 1)
    scale = HD ** -0.5
    for h in range(2):
        cl = pl.ds(h * HD, HD)
        of_row[h] = jnp.where(
            (lane_n % 8 == rank_col[:, 0:HD].astype(I32) + 4 * h) & (lane_n < 24), 1.0, 0.0).astype(F32)
        place[h] = jnp.where(spot_row == spot_col + 4 * h, 1.0, 0.0).astype(BF16)
        own = jnp.sum(fresh[0, :, cl].astype(F32) * fresh[1, :, cl].astype(F32), axis=1, keepdims=True) * scale
        own_sc[h] = jnp.broadcast_to(own, (n, HD))

    keep[0].wait()
    whole(*dat_x).wait_recv()
    got_ids = recv[:, 4].reshape(groups * 2, 128).astype(F32)
    slot = lax.broadcasted_iota(I32, (n, 128), 0) + 1
    half = (lax.broadcasted_iota(I32, (n, 128), 1) % 8) // 4
    for b in range(groups // 16):
        hit = jnp.sum(got_ids[32 * b:32 * b + 32], axis=0, keepdims=True).astype(I32) == slot
        for h in range(2):
            match[h, :, b * 128:(b + 1) * 128] = jnp.where(hit & (half == h), 1.0, 0.0).astype(BF16)
    arrived = recv[:, 0:4].reshape(groups * 8, HD)
    for h in range(2):
        owned[h] = dot(match[h], arrived).astype(BF16)

    kv_cp.wait()
    blocks = n // 16
    lane_i = lax.broadcasted_iota(I32, (n, 16 * length), 1)
    row_i = lax.broadcasted_iota(I32, (n, 16 * length), 0)
    valid = (lane_i // length == row_i % 16) & ((lane_i % length).astype(F32) < lengths)
    none = jnp.zeros((16, HD), BF16)
    for i in range(blocks):
        rows = slice(16 * i, 16 * i + 16)
        query = jnp.concatenate([
            jnp.concatenate([owned[0, rows], none], axis=1), jnp.concatenate([none, owned[1, rows]], axis=1)], axis=0)
        both = dot(query, kv[rows, 0].reshape(16 * length, 2 * HD), 1, 1)
        score[0, rows] = both[0:16]
        score[1, rows] = both[16:32]
    lse_of, weights = [], []
    for h in range(2):
        s = jnp.where(valid, score[h] * scale, -1e30)
        top = jnp.max(s, axis=1, keepdims=True)
        e = jnp.where(valid, jnp.exp(s - top), 0.0)
        total = jnp.sum(e, axis=1, keepdims=True)
        weights.append((e * (1.0 / total)).astype(BF16))
        lse_of.append(top + jnp.log(total))
    for i in range(blocks):
        rows = slice(16 * i, 16 * i + 16)
        both = dot(jnp.concatenate([weights[0][rows], weights[1][rows]], axis=0), kv[rows, 1].reshape(16 * length, 2 * HD))
        att[0, rows] = both[0:16, 0:HD].astype(BF16)
        att[1, rows] = both[16:32, HD:2 * HD].astype(BF16)
    lse_row = jnp.sum(
        match[0].astype(F32) * lse_of[0] + match[1].astype(F32) * lse_of[1], axis=0, keepdims=True)
    back = dot(match[0], att[0], 0, 0) + dot(match[1], att[1], 0, 0)
    rsend[:, 0:4] = back.astype(BF16).reshape(groups, 4, 2, HD)
    spread = jnp.zeros((groups, 128), F32)
    group_i = lax.broadcasted_iota(I32, (groups, 128), 0)
    for b in range(groups // 16):
        spread = jnp.where(group_i // 16 == b, lse_row[:, b * 128:(b + 1) * 128], spread)
    lse_rows = jnp.zeros((groups, 128), F32)
    for i in range(8):
        value = jnp.sum(jnp.where(lane == (group_i % 16) * 8 + i, spread, 0.0), axis=1, keepdims=True)
        lse_rows = jnp.where(lane % 8 == i, value, lse_rows)
    high = lse_rows.astype(BF16).astype(F32)
    middle = (lse_rows - high).astype(BF16).astype(F32)
    low = lse_rows - high - middle
    terms = jnp.where(lane < 8, high, jnp.where(lane < 16, middle, jnp.where(lane < 24, low, 0.0)))
    rsend[:, 4] = fifth(terms)

    each_peer(lambda to: to_peer(*ret_x, to).start())
    keep[1].start()

    pass_own(0)
    pass_own(1)

    keep[1].wait()
    whole(*ret_x).wait_recv()
    pieces = 4
    hr = n // pieces

    def ring_copy(s, q, way):
        src = lax.rem(y + (ring - s if way > 0 else s), ring)
        to = lax.rem(y + (1 if way > 0 else ring - 1), ring)
        at = gath.at[src, pl.ds(q * hr, hr)]
        i = (s * pieces + q) * 2 + (way > 0)
        return pltpu.make_async_remote_copy(
            at, at, ag_s, ag_r.at[i], device_id={"tensor": to}, device_id_type=MESH)

    last = ring // 2 - 1
    moves = [(s, q if way > 0 else pieces - 1 - q, way)
             for s in range(last + 1) for q in range(pieces) for way in (1, -1)
             if s < last or q < pieces // 2]
    back_rows = rrecv[:, 0:4].reshape(groups * 8, HD)
    term_rows = rrecv[:, 4].reshape(groups * 2, 128)

    def settle(q):
        rows = pl.ds(q * hr, hr)
        lse_terms = dot(of_owner[rows], term_rows)
        for h in range(2):
            cl = pl.ds(h * HD, HD)
            cached = dot(place[h, rows], back_rows)
            lse = jnp.sum(lse_terms * of_row[h, rows], axis=1, keepdims=True)
            own = own_sc[h, rows]
            top = jnp.maximum(lse, own)
            of_cache, of_own = jnp.exp(lse - top), jnp.exp(own - top)
            mixed = (of_cache * cached + of_own * fresh[2, rows, cl].astype(F32)) / (of_cache + of_own)
            gath[y, rows, cl] = (mixed * live[rows]).astype(BF16)

    settle(0)
    ring_copy(0, 0, 1).start()
    settle(3)
    ring_copy(0, 3, -1).start()
    settle(1)
    ring_copy(0, 1, 1).start()
    settle(2)
    ring_copy(0, 2, -1).start()
    for q in (2, 3):
        ring_copy(0, q, 1).start()
        ring_copy(0, 3 - q, -1).start()

    pass_sides(0)
    pass_sides(1)

    def relay(s):
        for m in moves:
            if m[0] == s:
                ring_copy(*m).wait_recv()
                nxt = (s + 1, m[1], m[2])
                if nxt in moves:
                    ring_copy(*nxt).start()

    def project(d):
        return dot(gath[lax.rem(y + ring - d, ring)], wcol[order.index(d)])

    relay(0)
    pass_last(0)
    pass_last(1)
    wown_cp.wait()
    res_cp.wait()
    acc[...] = res[...].astype(F32) + dot(gath[y], wcol[ring - 1])
    relay(1)
    w_all(wm_r.at[6], depth // 2, 0, ring - 1).wait_recv()
    acc[...] += project(1) + project(ring - 1)
    relay(2)
    acc[...] += project(2) + project(ring - 2)
    acc[...] += project(3) + project(ring - 3)
    farthest = lax.rem(y + ring // 2, ring)
    for m in moves:
        if m[0] == last:
            ring_copy(*m).wait_recv()
            rows = pl.ds(m[1] * hr, hr)
            done[rows] = (acc[rows] + dot(gath[farthest, rows], wcol[order.index(ring // 2)])).astype(BF16)
            pltpu.make_async_copy(done.at[rows], out_ref.at[rows], lsem.at[7]).start()

    for ex in (dat_x, ret_x):
        whole(*ex).wait_send()
    w_all(wm_r.at[6], depth, 0, ring - 1).wait_send()
    ring_all = gath.at[pl.ds(0, ring - 1)]
    pltpu.make_async_remote_copy(
        ring_all, ring_all, ag_s, ag_r.at[0], device_id={"tensor": y_peer(1)}, device_id_type=MESH).wait_send()
    pltpu.make_async_copy(done, out_ref, lsem.at[7]).wait()


def body(groups, ring, residual, fresh_qkv, active, home_slot, kv_cache, lengths, w_out):
    n = home_slot.shape[0]
    width = fresh_qkv.shape[2]
    cols = residual.shape[1]
    depth = w_out.shape[0]
    length = kv_cache.shape[2]
    hbm = pl.BlockSpec(memory_space=pl.ANY)
    dma = pltpu.SemaphoreType.DMA
    return pl.pallas_call(
        functools.partial(kernel, groups, ring),
        out_shape=jax.ShapeDtypeStruct((n, cols), BF16),
        in_specs=[hbm] * 7,
        out_specs=hbm,
        scratch_shapes=[
            pltpu.VMEM((3, n, width), BF16),
            pltpu.VMEM((3, 1, n), I32),
            pltpu.VMEM(kv_cache.shape, BF16),
            pltpu.VMEM((ring, depth, cols), BF16),
            pltpu.VMEM((n, cols), BF16),
            pltpu.VMEM((groups, 5, 2, HD), BF16),
            pltpu.VMEM((groups, 5, 2, HD), BF16),
            pltpu.VMEM((groups, 5, 2, HD), BF16),
            pltpu.VMEM((groups, 5, 2, HD), BF16),
            pltpu.VMEM((ring, n, width), BF16),
            pltpu.VMEM((2, n, groups * 8), BF16),
            pltpu.VMEM((2, n, groups * 8), BF16),
            pltpu.VMEM((2, n, HD), BF16),
            pltpu.VMEM((2, n, 16 * length), F32),
            pltpu.VMEM((2, n, HD), BF16),
            pltpu.VMEM((2, n, HD), F32),
            pltpu.VMEM((n, HD), F32),
            pltpu.VMEM((n, HD), BF16),
            pltpu.VMEM((2, n, HD), F32),
            pltpu.VMEM((n, cols), F32),
            pltpu.VMEM((n, cols), BF16),
            dma((8,)),
            dma, dma, dma, dma,
            dma, dma((2,)), dma((7,)), dma, dma((32,)),
        ],
        compiler_params=pltpu.CompilerParams(collective_id=0, has_side_effects=True),
    )(
        fresh_qkv.transpose(1, 0, 2), active.reshape(1, n), home_slot.reshape(1, n), lengths.reshape(1, n),
        kv_cache, w_out, residual,
    )


def solution(mesh):
    placed = (
        P("dp", "tensor"),
        P("dp", None, "tensor"),
        P("dp"),
        P("dp"),
        P("dp", None, None, "tensor"),
        P("dp"),
        P("tensor", None),
    )
    return jax.shard_map(
        functools.partial(body, mesh.shape["dp"], mesh.shape["tensor"]),
        mesh=mesh, in_specs=placed, out_specs=P("dp", "tensor"), check_vma=False,
    )
```

```python
import functools

import jax
import jax.numpy as jnp
from jax import lax
from jax.experimental import pallas as pl
from jax.experimental.pallas import tpu as pltpu
from jax.sharding import PartitionSpec as P

MESH = pl.DeviceIdType.MESH
HD = 128
CAP = 4
F32, BF16, I32 = jnp.float32, jnp.bfloat16, jnp.int32


def dot(a, b, ca=1, cb=0):
    return lax.dot_general(a, b, (((ca,), (cb,)), ((), ())), preferred_element_type=F32)


def kernel(
    groups, ring,
    fresh_hbm, act_hbm, home_hbm, len_hbm, kv_hbm, w_hbm, res_hbm,
    out_ref,
    fresh, small, kv, wcol, res, send, recv, rsend, rrecv,
    gath, place, match, owned, score, att, own_sc, live, of_owner, of_row, acc,
    lsem, dat_ss, dat_rs, ret_ss, ret_rs, w_sem, wy_r, wm_r, ag_s, ag_r,
):
    n = small.shape[2]
    length = kv.shape[2]
    cols = wcol.shape[2]
    depth = wcol.shape[1]
    planes = groups // 8
    me = lax.axis_index("dp")
    y = lax.axis_index("tensor")
    z, x, core = me // 8, lax.rem(me, 8) // 2, lax.rem(me, 2)
    partner = me + 1 - 2 * core

    plane_at = [lax.rem(z + dz, planes) * 8 for dz in range(planes)]
    chip_at = [lax.rem(x + dx, 4) * 2 for dx in range(4)]
    hops = lambda dz, dx: min(dz, planes - dz) + min(dx, 4 - dx)
    far_first = sorted(
        ((dz, dx) for dz in range(planes) for dx in range(4)),
        key=lambda p: (-hops(*p), abs(p[0] - planes // 2)))

    def each_peer(act):
        for dz, dx in far_first[:-1]:
            for c in range(2):
                act(plane_at[dz] + chip_at[dx] + c)
        act(partner)

    def y_peer(d):
        return lax.rem(y + d, ring)

    barrier = pltpu.get_barrier_semaphore()

    def greet(to):
        pl.semaphore_signal(barrier, inc=1, device_id={"dp": to}, device_id_type=MESH)

    for i, a in enumerate((home_hbm, act_hbm, len_hbm)):
        pltpu.make_async_copy(a, small.at[i], lsem.at[0]).start()
    fresh_cp = pltpu.make_async_copy(fresh_hbm, fresh, lsem.at[1])
    fresh_cp.start()
    each_peer(greet)
    for d in range(1, ring):
        pl.semaphore_signal(barrier, inc=1, device_id={"tensor": y_peer(d)}, device_id_type=MESH)
    kv_cp = pltpu.make_async_copy(kv_hbm, kv, lsem.at[2])
    kv_cp.start()
    wown_cp = pltpu.make_async_copy(
        w_hbm.at[:, pl.ds(pl.multiple_of(y * cols, cols), cols)], wcol.at[ring - 1], lsem.at[3])
    wown_cp.start()
    res_cp = pltpu.make_async_copy(res_hbm, res, lsem.at[4])
    res_cp.start()

    pltpu.make_async_copy(small, small, lsem.at[0]).wait()
    home = small[0]
    active = small[1] > 0
    owner = home // n
    local_id = (home - owner * n + 1).astype(F32)
    of_group = (owner == lax.broadcasted_iota(I32, (groups, n), 0)) & active
    one_hot = jnp.where(of_group, 1.0, 0.0).astype(F32)
    before = jnp.where(
        lax.broadcasted_iota(I32, (n, n), 0) < lax.broadcasted_iota(I32, (n, n), 1), 1.0, 0.0
    ).astype(BF16)
    earlier = dot(one_hot.astype(BF16), before)
    rank = jnp.sum(one_hot * earlier, axis=0, keepdims=True)
    lane = lax.broadcasted_iota(I32, (groups, 128), 1)
    mine = (lane // 8) == lax.rem(me, 16)
    id_rows = jnp.zeros((groups, 128), F32)
    for r in range(CAP):
        value = jnp.sum(jnp.where(rank == r, one_hot * local_id, 0.0), axis=1, keepdims=True)
        id_rows = jnp.where(mine & (lane % 4 == r), value, id_rows)
    first_row = lax.broadcasted_iota(I32, (groups, 2, 128), 1) == 0

    def fifth(rows):
        return jnp.where(first_row, jnp.broadcast_to(rows.reshape(groups, 1, 128), (groups, 2, 128)), 0.0).astype(BF16)

    send[:, 4] = fifth(id_rows)
    target = jnp.where(active, owner * 8 + rank.astype(I32), -64)
    spot = lax.broadcasted_iota(I32, (groups * 8, n), 0)
    fresh_cp.wait()
    rows = jnp.zeros((groups * 8, HD), F32)
    for h in range(2):
        rows += dot(jnp.where(spot == target + 4 * h, 1.0, 0.0).astype(BF16), fresh[0, :, h * HD:(h + 1) * HD])
    send[:, 0:4] = rows.astype(BF16).reshape(groups, 4, 2, HD)

    pl.semaphore_wait(barrier, groups - 1 + ring - 1)

    piece = depth // 8
    order = [1, 7, 2, 6, 3, 5, 4]
    parts = ((0, 4), (4, 3))

    def piece_of(dx):
        return (lax.rem(x + dx + 4, 4) * 2 + core) * piece

    def wy_copy(p):
        to = y_peer(order[p])
        rows = pl.ds(pl.multiple_of(piece_of(0), piece), piece)
        return pltpu.make_async_remote_copy(
            w_hbm.at[rows, pl.ds(pl.multiple_of(to * cols, cols), cols)], wcol.at[p, rows],
            w_sem, wy_r.at[int(p >= parts[1][0])], device_id={"tensor": to}, device_id_type=MESH)

    def wmove(kind, g):
        slot_of = (0, 2, 4, 4, 6, 6, 6, 6)
        to_x = lambda dx: z * 8 + lax.rem(x + dx + 4, 4) * 2 + core
        dx, start, size, to = (
            (0, 0, piece, to_x(1)), (0, 0, piece, to_x(-1)),
            (-1, 0, piece // 2, to_x(1)), (1, piece // 2, piece // 2, to_x(-1)),
            (0, 0, piece, partner), (-1, 0, piece, partner), (1, 0, piece, partner), (2, 0, piece, partner),
        )[kind]
        at = wcol.at[pl.ds(*parts[g]), pl.ds(pl.multiple_of(piece_of(dx) + start, size), size)]
        return pltpu.make_async_remote_copy(
            at, at, w_sem, wm_r.at[slot_of[kind] + (g if kind < 4 else 0)], device_id={"dp": to}, device_id_type=MESH)

    def w_all(recv_sem, rows, first, count):
        at = wcol.at[pl.ds(first, count), pl.ds(0, rows)]
        return pltpu.make_async_remote_copy(
            at, at, w_sem, recv_sem, device_id={"dp": partner}, device_id_type=MESH)

    def pass_own(g):
        w_all(wy_r.at[g], piece, *parts[g]).wait_recv()
        for kind in (0, 1, 4):
            wmove(kind, g).start()

    def pass_sides(g):
        for side in (0, 1):
            wmove(side, g).wait_recv()
            wmove(2 + side, g).start()
            wmove(5 + side, g).start()

    def pass_last(g):
        w_all(wm_r.at[4 + g], piece, *parts[g]).wait_recv()
        wmove(7, g).start()

    def to_peer(src, dst, ss, rs, to):
        return pltpu.make_async_remote_copy(
            src.at[to], dst.at[me], ss, rs, device_id={"dp": to}, device_id_type=MESH)

    def whole(src, dst, ss, rs):
        return pltpu.make_async_remote_copy(
            src.at[pl.ds(0, groups - 1)], dst.at[pl.ds(0, groups - 1)], ss, rs,
            device_id={"dp": partner}, device_id_type=MESH)

    dat_x = (send, recv, dat_ss, dat_rs)
    ret_x = (rsend, rrecv, ret_ss, ret_rs)

    for p in range(ring - 1):
        wy_copy(p).start()
    each_peer(lambda to: to_peer(*dat_x, to).start())
    keep = [pltpu.make_async_copy(a.at[me], b.at[me], lsem.at[5 + i]) for i, (a, b) in enumerate(
        ((send, recv), (rsend, rrecv)))]
    keep[0].start()

    eye = lax.broadcasted_iota(I32, (n, n), 0) == lax.broadcasted_iota(I32, (n, n), 1)

    def as_column(row, wide):
        return dot(jnp.where(eye, row, 0).astype(BF16), jnp.ones((n, wide), BF16))

    lengths = as_column(small[2].astype(F32), 16 * length)
    owner_col = as_column(jnp.where(active, owner, -8).astype(F32), groups * 8)
    rank_col = as_column(rank, groups * 8)
    spot_col = (owner_col * 8 + rank_col).astype(I32)
    lane_n = lax.broadcasted_iota(I32, (n, HD), 1)
    of_owner[...] = jnp.where(lane_n == owner_col[:, 0:HD].astype(I32) * 2, 1.0, 0.0).astype(BF16)
    live[...] = jnp.where(spot_col[:, 0:HD] >= 0, 1.0, 0.0)
    spot_row = lax.broadcasted_iota(I32, (n, groups * 8), 1)
    scale = HD ** -0.5
    for h in range(2):
        cl = pl.ds(h * HD, HD)
        of_row[h] = jnp.where(
            (lane_n % 8 == rank_col[:, 0:HD].astype(I32) + 4 * h) & (lane_n < 24), 1.0, 0.0).astype(F32)
        place[h] = jnp.where(spot_row == spot_col + 4 * h, 1.0, 0.0).astype(BF16)
        own = jnp.sum(fresh[0, :, cl].astype(F32) * fresh[1, :, cl].astype(F32), axis=1, keepdims=True) * scale
        own_sc[h] = jnp.broadcast_to(own, (n, HD))

    keep[0].wait()
    whole(*dat_x).wait_recv()
    got_ids = recv[:, 4].reshape(groups * 2, 128).astype(F32)
    slot = lax.broadcasted_iota(I32, (n, 128), 0) + 1
    half = (lax.broadcasted_iota(I32, (n, 128), 1) % 8) // 4
    for b in range(groups // 16):
        hit = jnp.sum(got_ids[32 * b:32 * b + 32], axis=0, keepdims=True).astype(I32) == slot
        for h in range(2):
            match[h, :, b * 128:(b + 1) * 128] = jnp.where(hit & (half == h), 1.0, 0.0).astype(BF16)
    arrived = recv[:, 0:4].reshape(groups * 8, HD)
    for h in range(2):
        owned[h] = dot(match[h], arrived).astype(BF16)

    kv_cp.wait()
    blocks = n // 16
    lane_i = lax.broadcasted_iota(I32, (n, 16 * length), 1)
    row_i = lax.broadcasted_iota(I32, (n, 16 * length), 0)
    valid = (lane_i // length == row_i % 16) & ((lane_i % length).astype(F32) < lengths)
    none = jnp.zeros((16, HD), BF16)
    for i in range(blocks):
        rows = slice(16 * i, 16 * i + 16)
        query = jnp.concatenate([
            jnp.concatenate([owned[0, rows], none], axis=1), jnp.concatenate([none, owned[1, rows]], axis=1)], axis=0)
        both = dot(query, kv[rows, 0].reshape(16 * length, 2 * HD), 1, 1)
        score[0, rows] = both[0:16]
        score[1, rows] = both[16:32]
    lse_of, weights = [], []
    for h in range(2):
        s = jnp.where(valid, score[h] * scale, -1e30)
        top = jnp.max(s, axis=1, keepdims=True)
        e = jnp.where(valid, jnp.exp(s - top), 0.0)
        total = jnp.sum(e, axis=1, keepdims=True)
        weights.append((e * (1.0 / total)).astype(BF16))
        lse_of.append(top + jnp.log(total))
    for i in range(blocks):
        rows = slice(16 * i, 16 * i + 16)
        both = dot(jnp.concatenate([weights[0][rows], weights[1][rows]], axis=0), kv[rows, 1].reshape(16 * length, 2 * HD))
        att[0, rows] = both[0:16, 0:HD].astype(BF16)
        att[1, rows] = both[16:32, HD:2 * HD].astype(BF16)
    lse_row = jnp.sum(
        match[0].astype(F32) * lse_of[0] + match[1].astype(F32) * lse_of[1], axis=0, keepdims=True)
    back = dot(match[0], att[0], 0, 0) + dot(match[1], att[1], 0, 0)
    rsend[:, 0:4] = back.astype(BF16).reshape(groups, 4, 2, HD)
    spread = jnp.zeros((groups, 128), F32)
    group_i = lax.broadcasted_iota(I32, (groups, 128), 0)
    for b in range(groups // 16):
        spread = jnp.where(group_i // 16 == b, lse_row[:, b * 128:(b + 1) * 128], spread)
    lse_rows = jnp.zeros((groups, 128), F32)
    for i in range(8):
        value = jnp.sum(jnp.where(lane == (group_i % 16) * 8 + i, spread, 0.0), axis=1, keepdims=True)
        lse_rows = jnp.where(lane % 8 == i, value, lse_rows)
    high = lse_rows.astype(BF16).astype(F32)
    middle = (lse_rows - high).astype(BF16).astype(F32)
    low = lse_rows - high - middle
    terms = jnp.where(lane < 8, high, jnp.where(lane < 16, middle, jnp.where(lane < 24, low, 0.0)))
    rsend[:, 4] = fifth(terms)

    each_peer(lambda to: to_peer(*ret_x, to).start())
    keep[1].start()

    pass_own(0)
    pass_own(1)

    keep[1].wait()
    whole(*ret_x).wait_recv()
    pieces = 4
    hr = n // pieces

    def ring_copy(s, q, way):
        src = lax.rem(y + (ring - s if way > 0 else s), ring)
        to = lax.rem(y + (1 if way > 0 else ring - 1), ring)
        at = gath.at[src, pl.ds(q * hr, hr)]
        i = (s * pieces + q) * 2 + (way > 0)
        return pltpu.make_async_remote_copy(
            at, at, ag_s, ag_r.at[i], device_id={"tensor": to}, device_id_type=MESH)

    last = ring // 2 - 1
    moves = [(s, q if way > 0 else pieces - 1 - q, way)
             for s in range(last + 1) for q in range(pieces) for way in (1, -1)
             if s < last or q < pieces // 2]
    back_rows = rrecv[:, 0:4].reshape(groups * 8, HD)
    term_rows = rrecv[:, 4].reshape(groups * 2, 128)

    def settle(q):
        rows = pl.ds(q * hr, hr)
        lse_terms = dot(of_owner[rows], term_rows)
        for h in range(2):
            cl = pl.ds(h * HD, HD)
            cached = dot(place[h, rows], back_rows)
            lse = jnp.sum(lse_terms * of_row[h, rows], axis=1, keepdims=True)
            own = own_sc[h, rows]
            top = jnp.maximum(lse, own)
            of_cache, of_own = jnp.exp(lse - top), jnp.exp(own - top)
            mixed = (of_cache * cached + of_own * fresh[2, rows, cl].astype(F32)) / (of_cache + of_own)
            gath[y, rows, cl] = (mixed * live[rows]).astype(BF16)

    settle(0)
    ring_copy(0, 0, 1).start()
    settle(3)
    ring_copy(0, 3, -1).start()
    settle(1)
    ring_copy(0, 1, 1).start()
    settle(2)
    ring_copy(0, 2, -1).start()
    for q in (2, 3):
        ring_copy(0, q, 1).start()
        ring_copy(0, 3 - q, -1).start()

    pass_sides(0)
    pass_sides(1)

    def relay(s):
        for m in moves:
            if m[0] == s:
                ring_copy(*m).wait_recv()
                nxt = (s + 1, m[1], m[2])
                if nxt in moves:
                    ring_copy(*nxt).start()

    def project(d):
        return dot(gath[lax.rem(y + ring - d, ring)], wcol[order.index(d)])

    relay(0)
    pass_last(0)
    pass_last(1)
    wown_cp.wait()
    res_cp.wait()
    acc[...] = res[...].astype(F32) + dot(gath[y], wcol[ring - 1])
    relay(1)
    w_all(wm_r.at[6], depth // 2, 0, ring - 1).wait_recv()
    acc[...] += project(1) + project(ring - 1)
    relay(2)
    acc[...] += project(2) + project(ring - 2)
    acc[...] += project(3) + project(ring - 3)
    farthest = lax.rem(y + ring // 2, ring)
    for m in moves:
        if m[0] == last:
            ring_copy(*m).wait_recv()
            rows = pl.ds(m[1] * hr, hr)
            out_ref[rows] = (acc[rows] + dot(gath[farthest, rows], wcol[order.index(ring // 2)])).astype(BF16)

    for ex in (dat_x, ret_x):
        whole(*ex).wait_send()
    w_all(wm_r.at[6], depth, 0, ring - 1).wait_send()
    ring_all = gath.at[pl.ds(0, ring - 1)]
    pltpu.make_async_remote_copy(
        ring_all, ring_all, ag_s, ag_r.at[0], device_id={"tensor": y_peer(1)}, device_id_type=MESH).wait_send()


def body(groups, ring, residual, fresh_qkv, active, home_slot, kv_cache, lengths, w_out):
    n = home_slot.shape[0]
    width = fresh_qkv.shape[2]
    cols = residual.shape[1]
    depth = w_out.shape[0]
    length = kv_cache.shape[2]
    hbm = pl.BlockSpec(memory_space=pl.ANY)
    dma = pltpu.SemaphoreType.DMA
    return pl.pallas_call(
        functools.partial(kernel, groups, ring),
        out_shape=pltpu.VMEM((n, cols), BF16),
        in_specs=[hbm] * 7,
        out_specs=pl.BlockSpec(memory_space=pltpu.VMEM),
        scratch_shapes=[
            pltpu.VMEM((3, n, width), BF16),
            pltpu.VMEM((3, 1, n), I32),
            pltpu.VMEM(kv_cache.shape, BF16),
            pltpu.VMEM((ring, depth, cols), BF16),
            pltpu.VMEM((n, cols), BF16),
            pltpu.VMEM((groups, 5, 2, HD), BF16),
            pltpu.VMEM((groups, 5, 2, HD), BF16),
            pltpu.VMEM((groups, 5, 2, HD), BF16),
            pltpu.VMEM((groups, 5, 2, HD), BF16),
            pltpu.VMEM((ring, n, width), BF16),
            pltpu.VMEM((2, n, groups * 8), BF16),
            pltpu.VMEM((2, n, groups * 8), BF16),
            pltpu.VMEM((2, n, HD), BF16),
            pltpu.VMEM((2, n, 16 * length), F32),
            pltpu.VMEM((2, n, HD), BF16),
            pltpu.VMEM((2, n, HD), F32),
            pltpu.VMEM((n, HD), F32),
            pltpu.VMEM((n, HD), BF16),
            pltpu.VMEM((2, n, HD), F32),
            pltpu.VMEM((n, cols), F32),
            dma((7,)),
            dma, dma, dma, dma,
            dma, dma((2,)), dma((7,)), dma, dma((32,)),
        ],
        compiler_params=pltpu.CompilerParams(collective_id=0, has_side_effects=True),
    )(
        fresh_qkv.transpose(1, 0, 2), active.reshape(1, n), home_slot.reshape(1, n), lengths.reshape(1, n),
        kv_cache, w_out, residual,
    )


def solution(mesh):
    placed = (
        P("dp", "tensor"),
        P("dp", None, "tensor"),
        P("dp"),
        P("dp"),
        P("dp", None, None, "tensor"),
        P("dp"),
        P("tensor", None),
    )
    return jax.shard_map(
        functools.partial(body, mesh.shape["dp"], mesh.shape["tensor"]),
        mesh=mesh, in_specs=placed, out_specs=P("dp", "tensor"), check_vma=False,
    )
```

```python
import functools

import jax
import jax.numpy as jnp
from jax import lax
from jax.experimental import pallas as pl
from jax.experimental.pallas import tpu as pltpu
from jax.sharding import PartitionSpec as P

MESH = pl.DeviceIdType.MESH
HD = 128
CAP = 4
F32, BF16, I32 = jnp.float32, jnp.bfloat16, jnp.int32


def dot(a, b, ca=1, cb=0):
    return lax.dot_general(a, b, (((ca,), (cb,)), ((), ())), preferred_element_type=F32)


def kernel(
    groups, ring,
    fresh_hbm, act_hbm, home_hbm, len_hbm, kv_hbm, w_hbm, res_hbm,
    out_ref,
    fresh, small, kv, wcol, res, send, recv, rsend, rrecv,
    gath, place, match, owned, score, att, own_sc, live, of_owner, of_row, bias, acc,
    lsem, dat_ss, dat_rs, ret_ss, ret_rs, w_sem, wy_r, wm_r, ag_s, ag_r,
):
    n = small.shape[2]
    length = kv.shape[2]
    cols = wcol.shape[2]
    depth = wcol.shape[1]
    planes = groups // 8
    me = lax.axis_index("dp")
    y = lax.axis_index("tensor")
    z, x, core = me // 8, lax.rem(me, 8) // 2, lax.rem(me, 2)
    partner = me + 1 - 2 * core

    plane_at = [lax.rem(z + dz, planes) * 8 for dz in range(planes)]
    chip_at = [lax.rem(x + dx, 4) * 2 for dx in range(4)]
    hops = lambda dz, dx: min(dz, planes - dz) + min(dx, 4 - dx)
    far_first = sorted(
        ((dz, dx) for dz in range(planes) for dx in range(4)),
        key=lambda p: (-hops(*p), abs(p[0] - planes // 2)))

    def each_peer(act):
        for dz, dx in far_first[:-1]:
            for c in range(2):
                act(plane_at[dz] + chip_at[dx] + c)
        act(partner)

    def y_peer(d):
        return lax.rem(y + d, ring)

    barrier = pltpu.get_barrier_semaphore()

    def greet(to):
        pl.semaphore_signal(barrier, inc=1, device_id={"dp": to}, device_id_type=MESH)

    for i, a in enumerate((home_hbm, act_hbm, len_hbm)):
        pltpu.make_async_copy(a, small.at[i], lsem.at[0]).start()
    fresh_cp = pltpu.make_async_copy(fresh_hbm, fresh, lsem.at[1])
    fresh_cp.start()
    each_peer(greet)
    for d in range(1, ring):
        pl.semaphore_signal(barrier, inc=1, device_id={"tensor": y_peer(d)}, device_id_type=MESH)
    kv_cp = pltpu.make_async_copy(kv_hbm, kv, lsem.at[2])
    kv_cp.start()
    wown_cp = pltpu.make_async_copy(
        w_hbm.at[:, pl.ds(pl.multiple_of(y * cols, cols), cols)], wcol.at[ring - 1], lsem.at[3])
    wown_cp.start()
    res_cp = pltpu.make_async_copy(res_hbm, res, lsem.at[4])
    res_cp.start()

    pltpu.make_async_copy(small, small, lsem.at[0]).wait()
    home = small[0]
    active = small[1] > 0
    owner = home // n
    local_id = (home - owner * n + 1).astype(F32)
    of_group = (owner == lax.broadcasted_iota(I32, (groups, n), 0)) & active
    one_hot = jnp.where(of_group, 1.0, 0.0).astype(F32)
    before = jnp.where(
        lax.broadcasted_iota(I32, (n, n), 0) < lax.broadcasted_iota(I32, (n, n), 1), 1.0, 0.0
    ).astype(BF16)
    earlier = dot(one_hot.astype(BF16), before)
    rank = jnp.sum(one_hot * earlier, axis=0, keepdims=True)
    lane = lax.broadcasted_iota(I32, (groups, 128), 1)
    mine = (lane // 8) == lax.rem(me, 16)
    id_rows = jnp.zeros((groups, 128), F32)
    for r in range(CAP):
        value = jnp.sum(jnp.where(rank == r, one_hot * local_id, 0.0), axis=1, keepdims=True)
        id_rows = jnp.where(mine & (lane % 4 == r), value, id_rows)
    first_row = lax.broadcasted_iota(I32, (groups, 2, 128), 1) == 0

    def fifth(rows):
        return jnp.where(first_row, jnp.broadcast_to(rows.reshape(groups, 1, 128), (groups, 2, 128)), 0.0).astype(BF16)

    send[:, 4] = fifth(id_rows)
    target = jnp.where(active, owner * 8 + rank.astype(I32), -64)
    spot = lax.broadcasted_iota(I32, (groups * 8, n), 0)
    fresh_cp.wait()
    rows = jnp.zeros((groups * 8, HD), F32)
    for h in range(2):
        rows += dot(jnp.where(spot == target + 4 * h, 1.0, 0.0).astype(BF16), fresh[0, :, h * HD:(h + 1) * HD])
    send[:, 0:4] = rows.astype(BF16).reshape(groups, 4, 2, HD)

    pl.semaphore_wait(barrier, groups - 1 + ring - 1)

    piece = depth // 8
    order = [1, 7, 2, 6, 3, 5, 4]
    parts = ((0, 4), (4, 3))

    def piece_of(dx):
        return (lax.rem(x + dx + 4, 4) * 2 + core) * piece

    def wy_copy(p):
        to = y_peer(order[p])
        rows = pl.ds(pl.multiple_of(piece_of(0), piece), piece)
        return pltpu.make_async_remote_copy(
            w_hbm.at[rows, pl.ds(pl.multiple_of(to * cols, cols), cols)], wcol.at[p, rows],
            w_sem, wy_r.at[int(p >= parts[1][0])], device_id={"tensor": to}, device_id_type=MESH)

    def wmove(kind, g):
        slot_of = (0, 2, 4, 4, 6, 6, 6, 6)
        to_x = lambda dx: z * 8 + lax.rem(x + dx + 4, 4) * 2 + core
        dx, start, size, to = (
            (0, 0, piece, to_x(1)), (0, 0, piece, to_x(-1)),
            (-1, 0, piece // 2, to_x(1)), (1, piece // 2, piece // 2, to_x(-1)),
            (0, 0, piece, partner), (-1, 0, piece, partner), (1, 0, piece, partner), (2, 0, piece, partner),
        )[kind]
        at = wcol.at[pl.ds(*parts[g]), pl.ds(pl.multiple_of(piece_of(dx) + start, size), size)]
        return pltpu.make_async_remote_copy(
            at, at, w_sem, wm_r.at[slot_of[kind] + (g if kind < 4 else 0)], device_id={"dp": to}, device_id_type=MESH)

    def w_all(recv_sem, rows, first, count):
        at = wcol.at[pl.ds(first, count), pl.ds(0, rows)]
        return pltpu.make_async_remote_copy(
            at, at, w_sem, recv_sem, device_id={"dp": partner}, device_id_type=MESH)

    def pass_own(g):
        w_all(wy_r.at[g], piece, *parts[g]).wait_recv()
        for kind in (0, 1, 4):
            wmove(kind, g).start()

    def pass_sides(g):
        for side in (0, 1):
            wmove(side, g).wait_recv()
            wmove(2 + side, g).start()
            wmove(5 + side, g).start()

    def pass_last(g):
        w_all(wm_r.at[4 + g], piece, *parts[g]).wait_recv()
        wmove(7, g).start()

    def to_peer(src, dst, ss, rs, to):
        return pltpu.make_async_remote_copy(
            src.at[to], dst.at[me], ss, rs, device_id={"dp": to}, device_id_type=MESH)

    def whole(src, dst, ss, rs):
        return pltpu.make_async_remote_copy(
            src.at[pl.ds(0, groups - 1)], dst.at[pl.ds(0, groups - 1)], ss, rs,
            device_id={"dp": partner}, device_id_type=MESH)

    dat_x = (send, recv, dat_ss, dat_rs)
    ret_x = (rsend, rrecv, ret_ss, ret_rs)

    for p in range(ring - 1):
        wy_copy(p).start()
    each_peer(lambda to: to_peer(*dat_x, to).start())
    keep = [pltpu.make_async_copy(a.at[me], b.at[me], lsem.at[5 + i]) for i, (a, b) in enumerate(
        ((send, recv), (rsend, rrecv)))]
    keep[0].start()

    eye = lax.broadcasted_iota(I32, (n, n), 0) == lax.broadcasted_iota(I32, (n, n), 1)

    def as_column(row, wide):
        return dot(jnp.where(eye, row, 0).astype(BF16), jnp.ones((n, wide), BF16))

    blocks = n // 16
    lane_i = lax.broadcasted_iota(I32, (n, 16 * length), 1)
    row_i = lax.broadcasted_iota(I32, (n, 16 * length), 0)
    lengths = as_column(small[2].astype(F32), 16 * length)
    valid = (lane_i // length == row_i % 16) & ((lane_i % length).astype(F32) < lengths)
    bias[...] = jnp.where(valid, 0.0, -1e30)
    owner_col = as_column(jnp.where(active, owner, -8).astype(F32), groups * 8)
    rank_col = as_column(rank, groups * 8)
    spot_col = (owner_col * 8 + rank_col).astype(I32)
    lane_n = lax.broadcasted_iota(I32, (n, HD), 1)
    of_owner[...] = jnp.where(lane_n == owner_col[:, 0:HD].astype(I32) * 2, 1.0, 0.0).astype(BF16)
    live[...] = jnp.where(spot_col[:, 0:HD] >= 0, 1.0, 0.0)
    spot_row = lax.broadcasted_iota(I32, (n, groups * 8), 1)
    scale = HD ** -0.5
    for h in range(2):
        cl = pl.ds(h * HD, HD)
        of_row[h] = jnp.where(
            (lane_n % 8 == rank_col[:, 0:HD].astype(I32) + 4 * h) & (lane_n < 24), 1.0, 0.0).astype(F32)
        place[h] = jnp.where(spot_row == spot_col + 4 * h, 1.0, 0.0).astype(BF16)
        own = jnp.sum(fresh[0, :, cl].astype(F32) * fresh[1, :, cl].astype(F32), axis=1, keepdims=True) * scale
        own_sc[h] = jnp.broadcast_to(own, (n, HD))

    keep[0].wait()
    whole(*dat_x).wait_recv()
    got_ids = recv[:, 4].reshape(groups * 2, 128).astype(F32)
    slot = lax.broadcasted_iota(I32, (n, 128), 0) + 1
    half = (lax.broadcasted_iota(I32, (n, 128), 1) % 8) // 4
    for b in range(groups // 16):
        hit = jnp.sum(got_ids[32 * b:32 * b + 32], axis=0, keepdims=True).astype(I32) == slot
        for h in range(2):
            match[h, :, b * 128:(b + 1) * 128] = jnp.where(hit & (half == h), 1.0, 0.0).astype(BF16)
    arrived = recv[:, 0:4].reshape(groups * 8, HD)
    for h in range(2):
        owned[h] = dot(match[h], arrived).astype(BF16)

    kv_cp.wait()
    none = jnp.zeros((16, HD), BF16)
    for i in range(blocks):
        rows = slice(16 * i, 16 * i + 16)
        query = jnp.concatenate([
            jnp.concatenate([owned[0, rows], none], axis=1), jnp.concatenate([none, owned[1, rows]], axis=1)], axis=0)
        both = dot(query, kv[rows, 0].reshape(16 * length, 2 * HD), 1, 1)
        score[0, rows] = both[0:16]
        score[1, rows] = both[16:32]
    weights, terms = [], []
    for h in range(2):
        s = score[h] * scale + bias[...]
        top = jnp.max(s, axis=1, keepdims=True)
        e = jnp.exp(s - top)
        total = jnp.sum(e, axis=1, keepdims=True)
        weights.append((e * (1.0 / total)).astype(BF16))
        lse = jnp.broadcast_to(top + jnp.log(total), (n, HD))
        high = lse.astype(BF16).astype(F32)
        middle = (lse - high).astype(BF16).astype(F32)
        low = lse - high - middle
        terms.append(jnp.where(
            lane_n < 8, high, jnp.where(lane_n < 16, middle, jnp.where(lane_n < 24, low, 0.0))).astype(BF16))
    for i in range(blocks):
        rows = slice(16 * i, 16 * i + 16)
        both = dot(jnp.concatenate([weights[0][rows], weights[1][rows]], axis=0), kv[rows, 1].reshape(16 * length, 2 * HD))
        att[0, rows] = both[0:16, 0:HD].astype(BF16)
        att[1, rows] = both[16:32, HD:2 * HD].astype(BF16)
    back = sum(
        dot(match[h], jnp.concatenate([att[h], terms[h]], axis=1), 0, 0) for h in range(2))
    rsend[:, 0:4] = back[:, 0:HD].astype(BF16).reshape(groups, 4, 2, HD)
    one_lane = lax.broadcasted_iota(I32, (groups * 8, HD), 1) % 8 == lax.broadcasted_iota(I32, (groups * 8, HD), 0) % 8
    rsend[:, 4] = fifth(jnp.sum(jnp.where(one_lane, back[:, HD:], 0.0).reshape(groups, 8, HD), axis=1))

    each_peer(lambda to: to_peer(*ret_x, to).start())
    keep[1].start()

    pass_own(0)
    pass_own(1)

    keep[1].wait()
    whole(*ret_x).wait_recv()
    pieces = 4
    hr = n // pieces

    def ring_copy(s, q, way):
        src = lax.rem(y + (ring - s if way > 0 else s), ring)
        to = lax.rem(y + (1 if way > 0 else ring - 1), ring)
        at = gath.at[src, pl.ds(q * hr, hr)]
        i = moves.index((s, q, way))
        return pltpu.make_async_remote_copy(
            at, at, ag_s, ag_r.at[i], device_id={"tensor": to}, device_id_type=MESH)

    last = ring // 2 - 1
    moves = [(s, q if way > 0 else pieces - 1 - q, way)
             for s in range(last + 1) for q in range(pieces) for way in (1, -1)
             if s < last or q < pieces // 2]
    back_rows = rrecv[:, 0:4].reshape(groups * 8, HD)
    term_rows = rrecv[:, 4].reshape(groups * 2, 128)

    def settle(q):
        rows = pl.ds(q * hr, hr)
        lse_terms = dot(of_owner[rows], term_rows)
        for h in range(2):
            cl = pl.ds(h * HD, HD)
            cached = dot(place[h, rows], back_rows)
            lse = jnp.sum(lse_terms * of_row[h, rows], axis=1, keepdims=True)
            own = own_sc[h, rows]
            top = jnp.maximum(lse, own)
            of_cache, of_own = jnp.exp(lse - top), jnp.exp(own - top)
            mixed = (of_cache * cached + of_own * fresh[2, rows, cl].astype(F32)) / (of_cache + of_own)
            gath[y, rows, cl] = (mixed * live[rows]).astype(BF16)

    settle(0)
    ring_copy(0, 0, 1).start()
    settle(3)
    ring_copy(0, 3, -1).start()
    settle(1)
    ring_copy(0, 1, 1).start()
    settle(2)
    ring_copy(0, 2, -1).start()
    for q in (2, 3):
        ring_copy(0, q, 1).start()
        ring_copy(0, 3 - q, -1).start()

    pass_sides(0)
    pass_sides(1)

    def relay(s):
        for m in moves:
            if m[0] == s:
                ring_copy(*m).wait_recv()
                nxt = (s + 1, m[1], m[2])
                if nxt in moves:
                    ring_copy(*nxt).start()

    def project(d):
        return dot(gath[lax.rem(y + ring - d, ring)], wcol[order.index(d)])

    relay(0)
    pass_last(0)
    pass_last(1)
    wown_cp.wait()
    res_cp.wait()
    acc[...] = res[...].astype(F32) + dot(gath[y], wcol[ring - 1])
    relay(1)
    w_all(wm_r.at[6], depth // 2, 0, ring - 1).wait_recv()
    acc[...] += project(1) + project(ring - 1)
    relay(2)
    acc[...] += project(2) + project(ring - 2)
    acc[...] += project(3) + project(ring - 3)
    farthest = lax.rem(y + ring // 2, ring)
    for m in moves:
        if m[0] == last:
            ring_copy(*m).wait_recv()
            rows = pl.ds(m[1] * hr, hr)
            out_ref[rows] = (acc[rows] + dot(gath[farthest, rows], wcol[order.index(ring // 2)])).astype(BF16)

    for ex in (dat_x, ret_x):
        whole(*ex).wait_send()
    w_all(wm_r.at[6], depth, 0, ring - 1).wait_send()
    ring_all = gath.at[pl.ds(0, ring - 1)]
    pltpu.make_async_remote_copy(
        ring_all, ring_all, ag_s, ag_r.at[0], device_id={"tensor": y_peer(1)}, device_id_type=MESH).wait_send()


def body(groups, ring, residual, fresh_qkv, active, home_slot, kv_cache, lengths, w_out):
    n = home_slot.shape[0]
    width = fresh_qkv.shape[2]
    cols = residual.shape[1]
    depth = w_out.shape[0]
    length = kv_cache.shape[2]
    hbm = pl.BlockSpec(memory_space=pl.ANY)
    dma = pltpu.SemaphoreType.DMA
    return pl.pallas_call(
        functools.partial(kernel, groups, ring),
        out_shape=pltpu.VMEM((n, cols), BF16),
        in_specs=[hbm] * 7,
        out_specs=pl.BlockSpec(memory_space=pltpu.VMEM),
        scratch_shapes=[
            pltpu.VMEM((3, n, width), BF16),
            pltpu.VMEM((3, 1, n), I32),
            pltpu.VMEM(kv_cache.shape, BF16),
            pltpu.VMEM((ring, depth, cols), BF16),
            pltpu.VMEM((n, cols), BF16),
            pltpu.VMEM((groups, 5, 2, HD), BF16),
            pltpu.VMEM((groups, 5, 2, HD), BF16),
            pltpu.VMEM((groups, 5, 2, HD), BF16),
            pltpu.VMEM((groups, 5, 2, HD), BF16),
            pltpu.VMEM((ring, n, width), BF16),
            pltpu.VMEM((2, n, groups * 8), BF16),
            pltpu.VMEM((2, n, groups * 8), BF16),
            pltpu.VMEM((2, n, HD), BF16),
            pltpu.VMEM((2, n, 16 * length), F32),
            pltpu.VMEM((2, n, HD), BF16),
            pltpu.VMEM((2, n, HD), F32),
            pltpu.VMEM((n, HD), F32),
            pltpu.VMEM((n, HD), BF16),
            pltpu.VMEM((2, n, HD), F32),
            pltpu.VMEM((n, 16 * length), F32),
            pltpu.VMEM((n, cols), F32),
            dma((7,)),
            dma, dma, dma, dma,
            dma, dma((2,)), dma((7,)), dma, dma((28,)),
        ],
        compiler_params=pltpu.CompilerParams(collective_id=0, has_side_effects=True),
    )(
        fresh_qkv.transpose(1, 0, 2), active.reshape(1, n), home_slot.reshape(1, n), lengths.reshape(1, n),
        kv_cache, w_out, residual,
    )


def solution(mesh):
    placed = (
        P("dp", "tensor"),
        P("dp", None, "tensor"),
        P("dp"),
        P("dp"),
        P("dp", None, None, "tensor"),
        P("dp"),
        P("tensor", None),
    )
    return jax.shard_map(
        functools.partial(body, mesh.shape["dp"], mesh.shape["tensor"]),
        mesh=mesh, in_specs=placed, out_specs=P("dp", "tensor"), check_vma=False,
    )
```
